512 devices in a mesh: gx: 32 (over y_hi, x, core), gy: 16 (over y_lo, z).
Axes of the slice: x: 4, y: 8 (y_hi: 4, y_lo: 2; y = y_hi * 2 + y_lo), z: 8, core: 2. Of those that a mesh axis runs over, the one named last changes fastest.
Arguments:
- node_values: bfloat16 [96, 48, 128, 256], P('gx', 'gy'), may hold values from -6 to 6
- fit_ops: bfloat16 [32, 16, 8, 320, 300], P('gx', 'gy'), may hold values from -0.0034179688 to 0.0034179688
- node_xyz: float32 [32, 16, 8, 3, 300], P('gx', 'gy'), may hold values from -6 to 6
- patch_nodes: int32 [32, 16, 8, 300], P('gx', 'gy'), may hold values from 0 to 3199, as said below
- patch_valid: int32 [32, 16, 8], P('gx', 'gy'), may hold values from 160 to 300
- patch_cell: int32 [32, 16, 8, 3], P('gx', 'gy'), may hold values from 0 to 11, as said below
- patch_radius: float32 [32, 16, 8], P('gx', 'gy'), may hold values from 3 to 6
- cell_scale: float32 [384, 192, 8], P('gx', 'gy'), may hold values from 0.5 to 2
Outputs:
- velocity: bfloat16 [384, 192, 8, 256], P('gx', 'gy')
The draws below stay inside these ranges and needn't reach their ends.
Inputs may be any that keep to these rules, and one draw needn't show every extreme that they name: `patch_nodes`: an entry (a * 5 + b) * 128 + n names node n of subregion (a, b) among the 5 by 5 subregions around the patch's tile, whose own subregions are a, b = 1 to 3; a and b differ by at most one from the subregion 1 + (3 c0) // 12, 1 + (3 c1) // 12 that holds the patch's centre cell, and the subregion never lies outside the grid along the second horizontal dimension. `patch_cell`: the first entry is below 12, the second below 12, the third at most 4.
All inputs are finite; a program needn't handle non-finite values.
Results may differ from the reference program's by a relative error of at most 0.0085.
Values may be sent and summed in bfloat16 or wider, within the bound.
A program may use at most 64 MiB of HBM per device.

```python
import math
import jax
import jax.numpy as jnp
import numpy as np
from jax import lax

K = 300
KP = 320
F = 256
NSUB = 128
PATCH_DEV = 8
CX = 12
CY = 12
CZ = 8
TILES_X = 32
TILES_Y = 16
NX = 384
NY = 192


def centres(key):
    base = jax.random.fold_in(key, 7)
    first_key, second_key, third_key = jax.random.split(base, 3)
    shape = (TILES_X, TILES_Y, PATCH_DEV)
    first = jax.random.randint(first_key, shape, 0, CX, dtype=jnp.int32)
    second = jax.random.randint(second_key, shape, 0, CY, dtype=jnp.int32)
    third = jax.random.randint(third_key, shape, 0, CZ - 3, dtype=jnp.int32)
    return (first, second, third)


def draw_patch_cell(key, part):
    first, second, third = centres(key)
    return jnp.stack([first, second, third], -1).astype(jnp.int32)


def draw_patch_nodes(key, part):
    first, second, third = centres(key)
    shape = (TILES_X, TILES_Y, PATCH_DEV, K)
    across_key, along_key, node_key = jax.random.split(jax.random.fold_in(key, 11), 3)
    home_x = 3 * first // CX
    home_y = 3 * second // CY
    sub_x = home_x[..., None] + jax.random.randint(across_key, shape, 0, 3, dtype=jnp.int32)
    sub_y = home_y[..., None] + jax.random.randint(along_key, shape, 0, 3, dtype=jnp.int32)
    tile_y = lax.broadcasted_iota(jnp.int32, shape, 1)
    lowest = jnp.where(tile_y == 0, 1, 0).astype(jnp.int32)
    highest = jnp.where(tile_y == TILES_Y - 1, 3, 4).astype(jnp.int32)
    sub_y = jnp.minimum(jnp.maximum(sub_y, lowest), highest)
    node = jax.random.randint(node_key, shape, 0, NSUB, dtype=jnp.int32)
    return ((sub_x * 5 + sub_y) * NSUB + node).astype(jnp.int32)


def set_ends(drawn, own_key, smallest, top_value):
    longest = drawn.shape.index(max(drawn.shape))
    spots = []
    for shift in (0, 1):
        where = [jax.random.randint(jax.random.fold_in(own_key, axis), (), 0, length) for axis, length in enumerate(drawn.shape)]
        where[longest] = (where[longest] + shift) % drawn.shape[longest]
        spots.append(tuple(where))
    return drawn.at[spots[0]].set(smallest).at[spots[1]].set(top_value)


def shard_levels(rng, shape, cuts, smallest, top_value):
    def one(position, parts):
        heights = jax.random.uniform(jax.random.fold_in(jax.random.fold_in(rng, 6), position), (parts,), jnp.float32, smallest / len(cuts), top_value / len(cuts))
        return jnp.repeat(jnp.exp(heights), shape[position] // parts).reshape((-1,) + (1,) * (len(shape) - position - 1))

    gain = one(*cuts[0])
    for cut in cuts[1:]:
        gain = gain * one(*cut)
    return gain


def noise(own_key, shape, spread, most, cuts=(), kind=jnp.bfloat16):
    result = jax.random.normal(own_key, shape, jnp.float32) * spread
    if len(cuts) > 0:
        result = shard_levels(own_key, shape, cuts, -0.22, 0.18) * result
    return jnp.clip(result, min=-most, max=most).astype(kind)


def setup_inputs(seed: int = 0) -> dict:
    key_list = jax.random.split(jax.random.key(seed), 9)
    return {
        "node_values": noise(key_list[0], (3 * TILES_X, 3 * TILES_Y, NSUB, F), 1.0, 6.0, ((0, 32), (1, 16))),
        "fit_ops": noise(key_list[1], (TILES_X, TILES_Y, PATCH_DEV, KP, K), (36 * K * K) ** -0.5, 0.0034179688, ((0, 32), (1, 16))),
        "node_xyz": jnp.clip(jax.random.uniform(key_list[2], (TILES_X, TILES_Y, PATCH_DEV, 3, K), jnp.float32, -6.0, 6.0) * shard_levels(key_list[2], (TILES_X, TILES_Y, PATCH_DEV, 3, K), ((0, 32), (1, 16)), -0.4, 0.0), -6.0, 6.0),
        "patch_nodes": draw_patch_nodes(jax.random.fold_in(key_list[8], 71), 0),
        "patch_valid": set_ends(jax.random.randint(key_list[4], (TILES_X, TILES_Y, PATCH_DEV), K // 2 + 10, K + 1), jax.random.fold_in(key_list[4], 1), K // 2 + 10, K).astype(jnp.int32),
        "patch_cell": draw_patch_cell(jax.random.fold_in(key_list[8], 71), 0),
        "patch_radius": jnp.clip(jnp.exp(math.log(6.0) - 0.6931472 * jax.random.uniform(key_list[6], (TILES_X, TILES_Y, PATCH_DEV), jnp.float32) ** shard_levels(key_list[6], (TILES_X, TILES_Y, PATCH_DEV), ((0, 32), (1, 16)), -0.2, 0.2)), 3.0, 6.0),
        "cell_scale": jnp.clip(jnp.exp(math.log(2.0) - 1.3862944 * jax.random.uniform(key_list[7], (NX, NY, CZ), jnp.float32) ** shard_levels(key_list[7], (NX, NY, CZ), ((0, 32), (1, 16)), -0.2, 0.2)), 0.5, 2.0),
    }


EXPONENTS = ((0, 0, 0), (1, 0, 0), (0, 1, 0), (0, 0, 1), (2, 0, 0), (1, 1, 0), (1, 0, 1), (0, 2, 0), (0, 1, 1), (0, 0, 2), (3, 0, 0), (2, 1, 0), (2, 0, 1), (1, 2, 0), (1, 1, 1), (1, 0, 2), (0, 3, 0), (0, 2, 1), (0, 1, 2), (0, 0, 3))

def stencil():
    across = np.arange(-4, 5).astype(np.float32)
    depth = np.arange(4).astype(np.float32) - 1.5
    first, second, third = np.meshgrid(across, across, depth, indexing='ij')
    return np.stack([first.ravel(), second.ravel(), third.ravel()], 1).astype(np.float32)

def patch_terms(gathered, operators, xyz, valid, radius):
    count = gathered.shape[0]
    fields = gathered.shape[2]
    slots = lax.broadcasted_iota(jnp.int32, gathered.shape[:2], 1)
    masked = jnp.where((slots < valid[:, None])[:, :, None], gathered, jnp.zeros((), gathered.dtype))
    coeffs = jnp.einsum('pik,pkf->pif', operators.astype(jnp.float32), masked.astype(jnp.float32), precision=lax.Precision.HIGHEST).astype(jnp.bfloat16)
    points = jnp.asarray(stencil())
    inverse = 1.0 / radius
    squared = jnp.zeros((count, points.shape[0], xyz.shape[2]), jnp.float32)
    for component in range(3):
        offset = points[None, :, component, None] - xyz[:, None, component, :]
        squared = squared + offset * offset
    scaled = squared * (inverse * inverse)[:, None, None]
    kernel = scaled * jnp.sqrt(scaled)
    unit_points = points[None, :, :] * inverse[:, None, None]
    powers = [jnp.ones_like(unit_points), unit_points, unit_points * unit_points, unit_points * unit_points * unit_points]
    monomials = [powers[first][..., 0] * powers[second][..., 1] * powers[third][..., 2] for first, second, third in EXPONENTS]
    design = jnp.concatenate([kernel, jnp.stack(monomials, -1)], -1).astype(jnp.bfloat16)
    values = jnp.einsum('pmi,pif->pmf', design.astype(jnp.float32), coeffs.astype(jnp.float32), precision=lax.Precision.HIGHEST)
    distance = jnp.sqrt(lax.optimization_barrier(jnp.sum(points * points, 1)))[None, :] * inverse[:, None]
    blend = jnp.maximum(1.0 - distance, 0.0) ** 4 * (4.0 * distance + 1.0)
    terms = values * blend[:, :, None]
    return terms.reshape(count, 9, 9, 4, fields)

def reference(node_values, fit_ops, node_xyz, patch_nodes, patch_valid, patch_cell, patch_radius, cell_scale):
    fields = node_values.shape[3]
    padded = jnp.pad(node_values, ((0, 0), (1, 1), (0, 0), (0, 0)))
    tiles = TILES_X * TILES_Y

    def tile_step(grid, inputs):
        tile_id, operators, xyz, indices, valid, cells, radius = inputs
        tile_x = tile_id // TILES_Y
        tile_y = tile_id % TILES_Y
        rows = (3 * tile_x - 1 + jnp.arange(5, dtype=jnp.int32)) % (3 * TILES_X)
        window = lax.dynamic_slice_in_dim(jnp.take(padded, rows, axis=0), 3 * tile_y, 5, 1)
        flat = window.reshape(25 * window.shape[2], fields)
        gathered = jnp.take(flat, indices, axis=0)
        terms = patch_terms(gathered, operators, xyz, valid, radius)
        anchor = jnp.stack([tile_x * CX, tile_y * CY, jnp.zeros((), jnp.int32)]).astype(jnp.int32)
        zero = jnp.zeros((), jnp.int32)

        def place(index, acc):
            start = (cells[index] + anchor).astype(jnp.int32)
            corner = (start[0], start[1], start[2], zero)
            block = lax.dynamic_slice(acc, corner, terms.shape[1:])
            return lax.dynamic_update_slice(acc, block + terms[index], corner)
        return (lax.fori_loop(0, PATCH_DEV, place, grid), None)
    start_grid = jnp.zeros((NX + 8, NY + 8, CZ, fields), jnp.float32)
    inputs = (jnp.arange(tiles, dtype=jnp.int32), fit_ops.reshape((tiles,) + fit_ops.shape[2:]), node_xyz.reshape((tiles,) + node_xyz.shape[2:]), patch_nodes.reshape((tiles,) + patch_nodes.shape[2:]), patch_valid.reshape((tiles,) + patch_valid.shape[2:]), patch_cell.reshape((tiles,) + patch_cell.shape[2:]), patch_radius.reshape((tiles,) + patch_radius.shape[2:]))
    grid, unused = lax.scan(tile_step, start_grid, inputs)
    folded = grid[4:NX + 4]
    folded = folded.at[:4].add(grid[NX + 4:NX + 8])
    folded = folded.at[NX - 4:].add(grid[:4])
    folded = folded[:, 4:NY + 4]
    return (cell_scale[..., None] * folded).astype(jnp.bfloat16)
```

```python
import functools

import jax
import jax.numpy as jnp
from jax import lax
from jax.experimental import pallas as pl
from jax.experimental.pallas import tpu as pltpu
from jax.sharding import PartitionSpec as P

EXPONENTS = (
    (0, 0, 0),
    (1, 0, 0),
    (0, 1, 0),
    (0, 0, 1),
    (2, 0, 0),
    (1, 1, 0),
    (1, 0, 1),
    (0, 2, 0),
    (0, 1, 1),
    (0, 0, 2),
    (3, 0, 0),
    (2, 1, 0),
    (2, 0, 1),
    (1, 2, 0),
    (1, 1, 1),
    (1, 0, 2),
    (0, 3, 0),
    (0, 2, 1),
    (0, 1, 2),
    (0, 0, 3),
)

K = 300
KS = 304
KP = 320
KL = 384
NSUB = 128
PATCHES = 8
SLAB = 48
BF = jnp.bfloat16
F32 = jnp.float32


def remote(src, dst, send, recv, axis, target):
    return pltpu.make_async_remote_copy(
        src_ref=src,
        dst_ref=dst,
        send_sem=send,
        recv_sem=recv,
        device_id={axis: target},
        device_id_type=pl.DeviceIdType.MESH,
    )


def kernel(
    nx,
    ny,
    nodes_hbm,
    fit_hbm,
    xyz_hbm,
    idx_hbm,
    scale_hbm,
    cell_ref,
    valid_ref,
    radius_ref,
    out_ref,
    nbr,
    fit_v,
    xyz_v,
    idx_v,
    scale_v,
    xyz_p,
    idx_b,
    ops_f,
    design,
    weights,
    onehot,
    place,
    slabs,
    acc,
    sxc,
    sxm,
    sz,
    rxc,
    rxm,
    rz,
    local_sem,
    hz_send,
    hz_recv,
    hx_send,
    hx_recv,
    hf_send,
    hf_recv,
    cc_send,
    cc_recv,
    cm_send,
    cm_recv,
    cz_send,
    cz_recv,
):
    gx, gy = lax.axis_index("gx"), lax.axis_index("gy")
    left, right = lax.rem(gx + nx - 1, nx), lax.rem(gx + 1, nx)
    sides_x = (left, right)
    has = (gy > 0, gy < ny - 1)
    sides_y = (jnp.maximum(gy - 1, 0), jnp.minimum(gy + 1, ny - 1))

    barrier = pltpu.get_barrier_semaphore()
    for side in sides_x:
        pl.semaphore_signal(
            barrier, inc=1, device_id={"gx": side}, device_id_type=pl.DeviceIdType.MESH
        )
    for d in range(2):

        @pl.when(has[d])
        def _():
            pl.semaphore_signal(
                barrier,
                inc=1,
                device_id={"gy": sides_y[d]},
                device_id_type=pl.DeviceIdType.MESH,
            )

    fetches = [
        pltpu.make_async_copy(idx_hbm, idx_v, local_sem.at[0]),
        pltpu.make_async_copy(xyz_hbm, xyz_v, local_sem.at[1]),
        pltpu.make_async_copy(fit_hbm, fit_v, local_sem.at[2]),
        pltpu.make_async_copy(scale_hbm, scale_v, local_sem.at[3]),
    ]
    for a in range(3):
        fetches.append(
            pltpu.make_async_copy(
                nodes_hbm.at[a], nbr.at[a + 1, pl.ds(1, 3)], local_sem.at[4 + a]
            )
        )
    for fetch in fetches:
        fetch.start()
    waits = 2 + jnp.where(gy > 0, 1, 0) + jnp.where(gy < ny - 1, 1, 0)
    pl.semaphore_wait(barrier, waits)

    def halo_y(d, a):
        return remote(
            nodes_hbm.at[a, 2 * d],
            nbr.at[a + 1, 4 - 4 * d],
            hz_send.at[d, a],
            hz_recv.at[d, a],
            "gy",
            sides_y[d],
        )

    def halo_x(d):
        return remote(
            nodes_hbm.at[2 * d],
            nbr.at[4 - 4 * d, pl.ds(1, 3)],
            hx_send.at[d],
            hx_recv.at[d],
            "gx",
            sides_x[d],
        )

    def halo_corner(e, d):
        return remote(
            nbr.at[1 + 2 * d, 4 * e],
            nbr.at[4 - 4 * d, 4 * e],
            hf_send.at[e, d],
            hf_recv.at[e, d],
            "gx",
            sides_x[d],
        )

    for a in (0, 2, 1):
        for d in range(2):

            @pl.when(has[d])
            def _():
                halo_y(d, a).start()

    for d in range(2):
        halo_x(d).start()

    for e in range(2):

        @pl.when(jnp.logical_not(has[e]))
        def _():
            for a in range(5):
                nbr[a, 4 * e] = jnp.zeros(nbr.shape[2:], BF)
            rz[1 - e] = jnp.zeros(rz.shape[1:], BF)

    fetches[0].wait()
    fetches[1].wait()
    xyz_p[...] = jnp.zeros(xyz_p.shape, F32)
    xyz_p[:, :, 0:K] = xyz_v[...]
    index = jnp.concatenate(
        [idx_v[...].astype(F32), jnp.zeros((PATCHES, KL - K), F32)], 1
    )
    columns = jnp.transpose(index)
    for p in range(PATCHES):
        idx_b[p] = jnp.broadcast_to(columns[0:KS, p : p + 1], (KS, 128)).astype(jnp.int32)

    for p in range(PATCHES):
        slabs[p, 9] = jnp.zeros((SLAB, slabs.shape[3]), BF)

    lane = lax.broadcasted_iota(jnp.int32, (1, KL), 1)
    owner, within = lane // SLAB, lane % SLAB
    target = jnp.zeros((1, KL), jnp.int32)
    for p in range(PATCHES):
        start = cell_ref[0, 1, 0, p] * 8 + cell_ref[0, 2, 0, p]
        target = jnp.where(owner == p, start, target)
    target = target + (within // 4) * 8 + within % 4
    target = jnp.where(within < 36, target, -1)
    rows = lax.broadcasted_iota(jnp.int32, (160, KL), 0)
    place[...] = jnp.where(rows == target, 1.0, 0.0).astype(BF)

    fetches[2].wait()
    for t in range(3):
        ops_f[t, K * 8 : KS * 8, :] = jnp.zeros(((KS - K) * 8, 128), F32)
    ops_f[2, :, 64:128] = jnp.zeros((KS * 8, 64), F32)

    def widen(i, carry):
        block = fit_v[pl.ds(i * 20, 20)].astype(F32).reshape(160, KP)
        at = pl.multiple_of(i * 160, 8)
        ops_f[0, pl.ds(at, 160), :] = block[:, 0:128]
        ops_f[1, pl.ds(at, 160), :] = block[:, 128:256]
        ops_f[2, pl.ds(at, 160), 0:64] = block[:, 256:320]
        return carry

    lax.fori_loop(0, K // 20, widen, 0)

    def prepare(p, carry):
        inverse = 1.0 / jnp.full((1, 128), radius_ref[0, 0, p], F32)
        inverse3 = jnp.concatenate([inverse] * 3, 1)
        x = xyz_p[0, pl.ds(p, 1), :] * inverse3
        y = xyz_p[1, pl.ds(p, 1), :] * inverse3
        z = xyz_p[2, pl.ds(p, 1), :] * inverse3
        row = lax.broadcasted_iota(jnp.int32, (SLAB, 128), 0)
        ey = (row // 4 - 4).astype(F32) * inverse
        ez = ((row % 4).astype(F32) - 1.5) * inverse
        ey3 = jnp.concatenate([ey] * 3, 1)
        ez3 = jnp.concatenate([ez] * 3, 1)
        away_yz = (ey3 - y) * (ey3 - y) + (ez3 - z) * (ez3 - z)
        flat = ey * ey + ez * ez
        tail = lax.broadcasted_iota(jnp.int32, (1, 128), 1) - (K - 256)

        def powers(base, which):
            result = jnp.zeros(jnp.broadcast_shapes(base.shape, (1, 128)), F32)
            raised = [jnp.ones_like(base), base, base * base, base * base * base]
            for power in range(4):
                hit = jnp.zeros((1, 128), jnp.bool_)
                for slot, exponent in enumerate(EXPONENTS):
                    if exponent[which] == power:
                        hit = hit | (tail == slot)
                result = jnp.where(hit, raised[power], result)
            return result

        mono_yz = powers(ey, 1) * powers(ez, 2)
        blends = []
        for i in range(9):
            ex = (i - 4) * inverse
            ex3 = jnp.concatenate([ex] * 3, 1)
            s = (ex3 - x) * (ex3 - x) + away_yz
            cubic = s * s * lax.rsqrt(jnp.maximum(s, 1e-30))
            mono = powers(ex, 0) * mono_yz
            last = jnp.where(tail < 0, cubic[:, 256:384], mono)
            design[SLAB * i : SLAB * i + SLAB, 0:256] = cubic[:, 0:256].astype(BF)
            design[SLAB * i : SLAB * i + SLAB, 256:384] = last.astype(BF)
            rho = jnp.sqrt(ex * ex + flat)
            rest = jnp.maximum(1.0 - rho, 0.0)
            rest = rest * rest
            blend = rest * rest * (4.0 * rho + 1.0)
            blends.append(jnp.where(row < 36, blend, 0.0))
        ops = jnp.concatenate(
            [ops_f[t, pl.ds(p, KS, stride=8), :].astype(BF) for t in range(3)], 1
        )
        ops = jnp.concatenate([ops, jnp.zeros((KL - KS, KL), BF)], 0)
        for i in range(9):
            w = lax.dot_general(
                design[SLAB * i : SLAB * i + SLAB, :],
                ops,
                (((1,), (1,)), ((), ())),
                preferred_element_type=F32,
            )
            weights[p, SLAB * i : SLAB * i + SLAB, :] = (
                w * jnp.concatenate([blends[i]] * 3, 1)
            ).astype(BF)

        entry = idx_b[p]
        sub = entry >> 7
        node = entry & 127
        a = (sub * 52) >> 8
        b = sub - 5 * a
        home = (cell_ref[0, 0, 0, p] // 4) * 3 + cell_ref[0, 1, 0, p] // 4
        block = a * 3 + b - home
        slot = lax.broadcasted_iota(jnp.int32, (KS, 128), 0)
        block = jnp.where(slot < valid_ref[0, 0, p], block, -1)
        match = jnp.where(
            node == lax.broadcasted_iota(jnp.int32, (KS, 128), 1), block, -1
        )
        for t in range(9):
            onehot[p, :, 128 * t : 128 * t + 128] = jnp.where(match == t, 1.0, 0.0).astype(BF)
        return carry

    lax.fori_loop(0, 4, prepare, 0)
    for e in range(2):

        @pl.when(has[e])
        def _():
            for d in range(2):
                halo_y(1 - e, 2 * d).wait_recv()
                halo_corner(e, d).start()

    lax.fori_loop(4, PATCHES, prepare, 0)

    for fetch in fetches[3:]:
        fetch.wait()
    for d in range(2):
        halo_x(d).wait_recv()
    for e in range(2):

        @pl.when(has[e])
        def _():
            halo_y(1 - e, 1).wait_recv()
            for d in range(2):
                halo_corner(e, d).wait_recv()

    def values(p, carry):
        home_x, home_y = cell_ref[0, 0, 0, p] // 4, cell_ref[0, 1, 0, p] // 4
        window = jnp.concatenate(
            [
                nbr[home_x + a, pl.ds(home_y, 3)].reshape(3 * NSUB, nbr.shape[3])
                for a in range(3)
            ],
            0,
        )
        samples = jnp.dot(onehot[p], window, preferred_element_type=F32).astype(BF)
        samples = jnp.concatenate(
            [samples, jnp.zeros((KL - KS, samples.shape[1]), BF)], 0
        )
        terms = jnp.dot(weights[p], samples, preferred_element_type=F32).astype(BF)
        slabs[p, 0:9] = terms.reshape(9, SLAB, terms.shape[1])
        return carry

    lax.fori_loop(0, PATCHES, values, 0)

    def reach(x):
        parts = []
        for p in range(PATCHES):
            at = x - cell_ref[0, 0, 0, p]
            at = jnp.where((at >= 0) & (at < 9), at, 9)
            parts.append(slabs[p, at])
        return jnp.dot(
            place[...], jnp.concatenate(parts, 0), preferred_element_type=F32
        )

    def send_corner(d, e):
        return remote(
            sxc.at[d, e], rxc.at[d, e], cc_send.at[d, e], cc_recv.at[d, e], "gx", sides_x[d]
        )

    def send_middle(d):
        return remote(sxm.at[d], rxm.at[d], cm_send.at[d], cm_recv.at[d], "gx", sides_x[d])

    def send_rows(d, part):
        return remote(
            sz.at[d, part],
            rz.at[d, part],
            cz_send.at[d, part],
            cz_recv.at[d, part],
            "gy",
            sides_y[d],
        )

    for d in range(2):

        def outer(i, carry):
            row = reach(16 * d + i)
            sxc[d, 0, i] = row[0:32].astype(BF)
            sxm[d, i] = row[32:128].astype(BF)
            sxc[d, 1, i] = row[128:160].astype(BF)
            return carry

        lax.fori_loop(0, 4, outer, 0)
        for e in range(2):
            send_corner(d, e).start()

    def inner(i, carry):
        acc[i] = reach(i + 4)
        return carry

    lax.fori_loop(4, 8, inner, 0)
    for e in range(2):
        sz[e, 1] = acc[4:8, 128 * e : 128 * e + 32].astype(BF)

        @pl.when(has[e])
        def _():
            send_rows(e, 1).start()

    for d in range(2):
        send_middle(d).start()
    lax.fori_loop(0, 4, inner, 0)
    lax.fori_loop(8, 12, inner, 0)

    for d in range(2):
        first = 8 - 8 * d
        for e in range(2):
            send_corner(d, e).wait_recv()
            sz[e, 2 - 2 * d] = (
                acc[first : first + 4, 128 * e : 128 * e + 32] + rxc[d, e].astype(F32)
            ).astype(BF)

            @pl.when(has[e])
            def _():
                send_rows(e, 2 - 2 * d).start()

    for d in range(2):
        send_middle(d).wait_recv()
        first = 8 - 8 * d
        acc[first : first + 4, 32:128] += rxm[d].astype(F32)

    for d in range(2):
        for part in range(3):

            @pl.when(has[1 - d])
            def _():
                send_rows(d, part).wait_recv()

    def finish(i, carry):
        factor = scale_v[i]
        part, at = i // 4, lax.rem(i, 4)
        for y in range(12):
            total = acc[i, 32 + 8 * y : 40 + 8 * y, :]
            if y >= 8:
                total += rz[0, part, at, 8 * (y - 8) : 8 * (y - 8) + 8, :].astype(F32)
            if y < 4:
                total += rz[1, part, at, 8 * y : 8 * y + 8, :].astype(F32)
            out_ref[i, y] = (factor[:, y : y + 1] * total).astype(BF)
        return carry

    lax.fori_loop(0, 12, finish, 0)

    for d in range(2):
        halo_x(d).wait_send()
        send_middle(d).wait_send()
        for e in range(2):
            send_corner(d, e).wait_send()

        @pl.when(has[d])
        def _():
            for a in range(3):
                halo_y(d, a).wait_send()
                send_rows(d, a).wait_send()
            for e in range(2):
                halo_corner(d, e).wait_send()


def fused(nx, ny, nodes, fit, xyz, idx, scale, cell, valid, radius):
    fields = nodes.shape[3]
    anywhere = pl.BlockSpec(memory_space=pl.ANY)
    scalars = pl.BlockSpec(memory_space=pltpu.SMEM)
    dma = pltpu.SemaphoreType.DMA
    return pl.pallas_call(
        functools.partial(kernel, nx, ny),
        out_shape=jax.ShapeDtypeStruct((12, 12, 8, fields), BF),
        in_specs=[anywhere] * 5 + [scalars] * 3,
        out_specs=pl.BlockSpec(memory_space=pltpu.VMEM),
        scratch_shapes=[
            pltpu.VMEM((5, 5, NSUB, fields), BF),
            pltpu.VMEM((K, PATCHES, KP), BF),
            pltpu.VMEM((3, PATCHES, K), F32),
            pltpu.VMEM((PATCHES, K), jnp.int32),
            pltpu.VMEM((12, 8, 12), F32),
            pltpu.VMEM((3, PATCHES, KL), F32),
            pltpu.VMEM((PATCHES, KS, 128), jnp.int32),
            pltpu.VMEM((3, KS * PATCHES, 128), F32),
            pltpu.VMEM((9 * SLAB, KL), BF),
            pltpu.VMEM((PATCHES, 9 * SLAB, KL), BF),
            pltpu.VMEM((PATCHES, KS, 9 * NSUB), BF),
            pltpu.VMEM((160, KL), BF),
            pltpu.VMEM((PATCHES, 10, SLAB, fields), BF),
            pltpu.VMEM((12, 160, fields), F32),
            pltpu.VMEM((2, 2, 4, 32, fields), BF),
            pltpu.VMEM((2, 4, 96, fields), BF),
            pltpu.VMEM((2, 3, 4, 32, fields), BF),
            pltpu.VMEM((2, 2, 4, 32, fields), BF),
            pltpu.VMEM((2, 4, 96, fields), BF),
            pltpu.VMEM((2, 3, 4, 32, fields), BF),
            dma((7,)),
            dma((2, 3)),
            dma((2, 3)),
            dma((2,)),
            dma((2,)),
            dma((2, 2)),
            dma((2, 2)),
            dma((2, 2)),
            dma((2, 2)),
            dma((2,)),
            dma((2,)),
            dma((2, 3)),
            dma((2, 3)),
        ],
        compiler_params=pltpu.CompilerParams(
            collective_id=0, has_side_effects=True, vmem_limit_bytes=56 * 1024 * 1024
        ),
        name="fit_and_blend",
    )(nodes, fit, xyz, idx, scale, cell, valid, radius)


def local(
    nx,
    ny,
    node_values,
    fit_ops,
    node_xyz,
    patch_nodes,
    patch_valid,
    patch_cell,
    patch_radius,
    cell_scale,
):
    return fused(
        nx,
        ny,
        node_values,
        jnp.transpose(fit_ops[0, 0], (2, 0, 1)),
        jnp.transpose(node_xyz[0, 0], (1, 0, 2)),
        patch_nodes[0, 0],
        jnp.transpose(cell_scale, (0, 2, 1)),
        jnp.transpose(patch_cell, (0, 3, 1, 2)),
        patch_valid,
        patch_radius,
    )


def solution(mesh):
    placed = (
        P("gx", "gy", None, None),
        P("gx", "gy", None, None, None),
        P("gx", "gy", None, None, None),
        P("gx", "gy", None, None),
        P("gx", "gy", None),
        P("gx", "gy", None, None),
        P("gx", "gy", None),
        P("gx", "gy", None),
    )
    return jax.shard_map(
        functools.partial(local, mesh.shape["gx"], mesh.shape["gy"]),
        mesh=mesh,
        in_specs=placed,
        out_specs=P("gx", "gy", None, None),
        check_vma=False,
    )
```

```python
import functools

import jax
import jax.numpy as jnp
from jax import lax
from jax.experimental import pallas as pl
from jax.experimental.pallas import tpu as pltpu
from jax.sharding import PartitionSpec as P

EXPONENTS = (
    (0, 0, 0),
    (1, 0, 0),
    (0, 1, 0),
    (0, 0, 1),
    (2, 0, 0),
    (1, 1, 0),
    (1, 0, 1),
    (0, 2, 0),
    (0, 1, 1),
    (0, 0, 2),
    (3, 0, 0),
    (2, 1, 0),
    (2, 0, 1),
    (1, 2, 0),
    (1, 1, 1),
    (1, 0, 2),
    (0, 3, 0),
    (0, 2, 1),
    (0, 1, 2),
    (0, 0, 3),
)

K = 300
KS = 304
KP = 320
KL = 384
NSUB = 128
PATCHES = 8
RUN = 8
SLAB = 48
BF = jnp.bfloat16
F32 = jnp.float32


def remote(src, dst, send, recv, axis, target):
    return pltpu.make_async_remote_copy(
        src_ref=src,
        dst_ref=dst,
        send_sem=send,
        recv_sem=recv,
        device_id={axis: target},
        device_id_type=pl.DeviceIdType.MESH,
    )


def kernel(
    nx,
    ny,
    nodes_hbm,
    fit_hbm,
    xyz_hbm,
    idx_hbm,
    scale_hbm,
    cell_hbm,
    valid_hbm,
    radius_hbm,
    out_ref,
    nbr,
    fit_v,
    xyz_v,
    idx_v,
    scale_v,
    xyz_p,
    idx_b,
    ops_f,
    design,
    weights,
    onehot,
    place,
    slabs,
    acc,
    sxc,
    sxm,
    sz,
    rxc,
    ryc,
    rxm,
    rz,
    out_v,
    cell_ref,
    valid_ref,
    radius_ref,
    local_sem,
    hz_send,
    hz_recv,
    hx_send,
    hx_recv,
    hf_send,
    hf_recv,
    hg_send,
    hg_recv,
    cc_send,
    cc_recv,
    cy_send,
    cy_recv,
    cm_send,
    cm_recv,
    cz_send,
    cz_recv,
    out_sem,
):
    gx, gy = lax.axis_index("gx"), lax.axis_index("gy")
    left, right = lax.rem(gx + nx - 1, nx), lax.rem(gx + 1, nx)
    sides_x = (left, right)
    far = (lax.rem(gx, RUN) == 0, lax.rem(gx, RUN) == RUN - 1)
    near = tuple(jnp.logical_not(f) for f in far)
    has = (gy > 0, gy < ny - 1)
    sides_y = (jnp.maximum(gy - 1, 0), jnp.minimum(gy + 1, ny - 1))

    barrier = pltpu.get_barrier_semaphore()
    for side in sides_x:
        pl.semaphore_signal(
            barrier, inc=1, device_id={"gx": side}, device_id_type=pl.DeviceIdType.MESH
        )
    for d in range(2):

        @pl.when(has[d])
        def _():
            pl.semaphore_signal(
                barrier,
                inc=1,
                device_id={"gy": sides_y[d]},
                device_id_type=pl.DeviceIdType.MESH,
            )

    fetches = [
        pltpu.make_async_copy(idx_hbm, idx_v, local_sem.at[0]),
        pltpu.make_async_copy(xyz_hbm, xyz_v, local_sem.at[1]),
        pltpu.make_async_copy(fit_hbm, fit_v, local_sem.at[2]),
        pltpu.make_async_copy(scale_hbm, scale_v, local_sem.at[3]),
        pltpu.make_async_copy(cell_hbm, cell_ref, local_sem.at[7]),
        pltpu.make_async_copy(valid_hbm, valid_ref, local_sem.at[8]),
        pltpu.make_async_copy(radius_hbm, radius_ref, local_sem.at[9]),
    ]
    for a in range(3):
        fetches.append(
            pltpu.make_async_copy(
                nodes_hbm.at[a], nbr.at[a + 1, pl.ds(1, 3)], local_sem.at[4 + a]
            )
        )
    for fetch in fetches:
        fetch.start()
    waits = 2 + jnp.where(gy > 0, 1, 0) + jnp.where(gy < ny - 1, 1, 0)
    pl.semaphore_wait(barrier, waits)

    def halo_y(d, a):
        return remote(
            nodes_hbm.at[a, 2 * d],
            nbr.at[a + 1, 4 - 4 * d],
            hz_send.at[d, a],
            hz_recv.at[d, a],
            "gy",
            sides_y[d],
        )

    def halo_x(d, b):
        return remote(
            nodes_hbm.at[2 * d, b],
            nbr.at[4 - 4 * d, b + 1],
            hx_send.at[d, b],
            hx_recv.at[d, b],
            "gx",
            sides_x[d],
        )

    def halo_corner(e, d):
        return remote(
            nbr.at[1 + 2 * d, 4 * e],
            nbr.at[4 - 4 * d, 4 * e],
            hf_send.at[e, d],
            hf_recv.at[e, d],
            "gx",
            sides_x[d],
        )

    def halo_corner_far(d, e):
        return remote(
            nbr.at[4 * d, 1 + 2 * e],
            nbr.at[4 * d, 4 - 4 * e],
            hg_send.at[d, e],
            hg_recv.at[d, e],
            "gy",
            sides_y[e],
        )

    for a in (0, 2, 1):
        for d in range(2):

            @pl.when(has[d])
            def _():
                halo_y(d, a).start()

        for d in range(2):
            halo_x(d, a).start()

    for e in range(2):

        @pl.when(jnp.logical_not(has[e]))
        def _():
            for a in range(5):
                nbr[a, 4 * e] = jnp.zeros(nbr.shape[2:], BF)
            rz[1 - e] = jnp.zeros(rz.shape[1:], BF)

    for i in (0, 1, 4, 5, 6):
        fetches[i].wait()
    xyz_p[...] = jnp.zeros(xyz_p.shape, F32)
    xyz_p[:, :, 0:K] = xyz_v[...]
    entry = jnp.concatenate(
        [idx_v[...], jnp.zeros((PATCHES, KL - K), jnp.int32)], 1
    )
    sub = entry >> 7
    a = (sub * 52) >> 8
    patch = lax.broadcasted_iota(jnp.int32, (PATCHES, KL), 0)
    home = jnp.zeros((PATCHES, KL), jnp.int32)
    count = jnp.zeros((PATCHES, KL), jnp.int32)
    for p in range(PATCHES):
        corner = (cell_ref[0, 0, 0, p] // 4) * 3 + cell_ref[0, 1, 0, p] // 4
        home = jnp.where(patch == p, corner, home)
        count = jnp.where(patch == p, valid_ref[0, 0, p], count)
    entry = ((sub - 2 * a - home) << 7) + (entry & 127)
    slot = lax.broadcasted_iota(jnp.int32, (PATCHES, KL), 1)
    entry = jnp.where(slot < count, entry, -1)
    columns = jnp.transpose(entry.astype(F32))
    for p in range(PATCHES):
        idx_b[p] = jnp.broadcast_to(columns[0:KS, p : p + 1], (KS, 128)).astype(jnp.int32)

    for p in range(PATCHES):
        slabs[p, 9] = jnp.zeros((SLAB, slabs.shape[3]), BF)

    lane = lax.broadcasted_iota(jnp.int32, (1, KL), 1)
    owner, within = lane // SLAB, lane % SLAB
    target = jnp.zeros((1, KL), jnp.int32)
    for p in range(PATCHES):
        start = cell_ref[0, 1, 0, p] * 8 + cell_ref[0, 2, 0, p]
        target = jnp.where(owner == p, start, target)
    target = target + (within // 4) * 8 + within % 4
    target = jnp.where(within < 36, target, -1)
    rows = lax.broadcasted_iota(jnp.int32, (160, KL), 0)
    place[...] = jnp.where(rows == target, 1.0, 0.0).astype(BF)

    fetches[2].wait()
    for t in range(3):
        ops_f[t, K * 8 : KS * 8, :] = jnp.zeros(((KS - K) * 8, 128), F32)
    ops_f[2, :, 64:128] = jnp.zeros((KS * 8, 64), F32)

    def widen(i, carry):
        block = fit_v[pl.ds(i * 20, 20)].astype(F32).reshape(160, KP)
        at = pl.multiple_of(i * 160, 8)
        ops_f[0, pl.ds(at, 160), :] = block[:, 0:128]
        ops_f[1, pl.ds(at, 160), :] = block[:, 128:256]
        ops_f[2, pl.ds(at, 160), 0:64] = block[:, 256:320]
        return carry

    lax.fori_loop(0, K // 20, widen, 0)

    def prepare(p, carry):
        inverse = 1.0 / jnp.full((1, 128), radius_ref[0, 0, p], F32)
        inverse3 = jnp.concatenate([inverse] * 3, 1)
        x = xyz_p[0, pl.ds(p, 1), :] * inverse3
        y = xyz_p[1, pl.ds(p, 1), :] * inverse3
        z = xyz_p[2, pl.ds(p, 1), :] * inverse3
        row = lax.broadcasted_iota(jnp.int32, (SLAB, 128), 0)
        ey = (row // 4 - 4).astype(F32) * inverse
        ez = ((row % 4).astype(F32) - 1.5) * inverse
        ey3 = jnp.concatenate([ey] * 3, 1)
        ez3 = jnp.concatenate([ez] * 3, 1)
        away_yz = (ey3 - y) * (ey3 - y) + (ez3 - z) * (ez3 - z)
        flat = ey * ey + ez * ez
        tail = lax.broadcasted_iota(jnp.int32, (1, 128), 1) - (K - 256)

        def powers(base, which):
            result = jnp.zeros(jnp.broadcast_shapes(base.shape, (1, 128)), F32)
            raised = [jnp.ones_like(base), base, base * base, base * base * base]
            for power in range(4):
                hit = jnp.zeros((1, 128), jnp.bool_)
                for slot, exponent in enumerate(EXPONENTS):
                    if exponent[which] == power:
                        hit = hit | (tail == slot)
                result = jnp.where(hit, raised[power], result)
            return result

        mono_yz = powers(ey, 1) * powers(ez, 2)
        ops = jnp.concatenate(
            [ops_f[t, pl.ds(p, KS, stride=8), :].astype(BF) for t in range(3)], 1
        )
        ops = jnp.concatenate([ops, jnp.zeros((KL - KS, KL), BF)], 0)
        for group in range(3):
            for i in range(3 * group, 3 * group + 3):
                ex = (i - 4) * inverse
                ex3 = jnp.concatenate([ex] * 3, 1)
                s = (ex3 - x) * (ex3 - x) + away_yz
                cubic = s * s * lax.rsqrt(jnp.maximum(s, 1e-30))
                mono = powers(ex, 0) * mono_yz
                last = jnp.where(tail < 0, cubic[:, 256:384], mono)
                design[SLAB * i : SLAB * i + SLAB, 0:256] = cubic[:, 0:256].astype(BF)
                design[SLAB * i : SLAB * i + SLAB, 256:384] = last.astype(BF)
            w = lax.dot_general(
                design[3 * SLAB * group : 3 * SLAB * group + 3 * SLAB, :],
                ops,
                (((1,), (1,)), ((), ())),
                preferred_element_type=F32,
            )
            for j in range(3):
                i = 3 * group + j
                ex = (i - 4) * inverse
                rho = jnp.sqrt(ex * ex + flat)
                rest = jnp.maximum(1.0 - rho, 0.0)
                rest = rest * rest
                blend = rest * rest * (4.0 * rho + 1.0)
                blend = jnp.where(row < 36, blend, 0.0)
                weights[p, SLAB * i : SLAB * i + SLAB, :] = (
                    w[SLAB * j : SLAB * j + SLAB] * jnp.concatenate([blend] * 3, 1)
                ).astype(BF)

        entry = idx_b[p]
        node = (entry & 127).astype(F32).astype(BF)
        block = (entry >> 7).astype(F32).astype(BF)
        lanes = lax.broadcasted_iota(jnp.int32, (KS, 128), 1).astype(F32).astype(BF)
        match = jnp.where(node == lanes, block, jnp.full((KS, 128), -1.0, BF))
        one, zero = jnp.full((KS, 128), 1.0, BF), jnp.zeros((KS, 128), BF)
        for t in range(9):
            onehot[p, :, 128 * t : 128 * t + 128] = jnp.where(
                match == jnp.full((KS, 128), t, BF), one, zero
            )
        return carry

    lax.fori_loop(0, 4, prepare, 0)
    for e in range(2):
        for d in range(2):

            @pl.when(has[e] & near[d])
            def _():
                halo_y(1 - e, 2 * d).wait_recv()
                halo_corner(e, d).start()

            @pl.when(has[e] & far[d])
            def _():
                halo_x(1 - d, 2 * e).wait_recv()
                halo_corner_far(d, e).start()

    lax.fori_loop(4, PATCHES, prepare, 0)

    for i in (3, 7, 8, 9):
        fetches[i].wait()
    for d in range(2):
        halo_x(d, 1).wait_recv()
        for e in range(2):
            @pl.when(near[1 - d] | jnp.logical_not(has[e]))
            def _():
                halo_x(d, 2 * e).wait_recv()

            @pl.when(has[e] & far[d])
            def _():
                halo_y(1 - e, 2 * d).wait_recv()

            @pl.when(has[e] & near[d])
            def _():
                halo_corner(e, 1 - d).wait_recv()

            @pl.when(has[e] & far[d])
            def _():
                halo_corner_far(d, 1 - e).wait_recv()

    for e in range(2):

        @pl.when(has[e])
        def _():
            halo_y(1 - e, 1).wait_recv()

    for p in range(PATCHES):
        home_x, home_y = cell_ref[0, 0, 0, p] // 4, cell_ref[0, 1, 0, p] // 4
        window = jnp.concatenate(
            [
                nbr[home_x + a, pl.ds(home_y, 3)].reshape(3 * NSUB, nbr.shape[3])
                for a in range(3)
            ],
            0,
        )
        samples = jnp.dot(onehot[p], window, preferred_element_type=F32).astype(BF)
        samples = jnp.concatenate(
            [samples, jnp.zeros((KL - KS, samples.shape[1]), BF)], 0
        )
        terms = jnp.dot(weights[p], samples, preferred_element_type=F32).astype(BF)
        slabs[p, 0:9] = terms.reshape(9, SLAB, terms.shape[1])

    def reach(x):
        parts = []
        for p in range(PATCHES):
            at = x - cell_ref[0, 0, 0, p]
            at = jnp.where((at >= 0) & (at < 9), at, 9)
            parts.append(slabs[p, at])
        return jnp.dot(
            place[...], jnp.concatenate(parts, 0), preferred_element_type=F32
        )

    def send_corner(d, e):
        return remote(
            sxc.at[d, e], rxc.at[d, e], cc_send.at[d, e], cc_recv.at[d, e], "gx", sides_x[d]
        )

    def send_corner_far(d, e):
        return remote(
            sxc.at[d, e], ryc.at[d, e], cy_send.at[d, e], cy_recv.at[d, e], "gy", sides_y[e]
        )

    def send_middle(d, part):
        return remote(
            sxm.at[d, part],
            rxm.at[d, part],
            cm_send.at[d, part],
            cm_recv.at[d, part],
            "gx",
            sides_x[d],
        )

    def send_rows(d, part):
        return remote(
            sz.at[d, part],
            rz.at[d, part],
            cz_send.at[d, part],
            cz_recv.at[d, part],
            "gy",
            sides_y[d],
        )

    for d in range(2):
        for i in range(4):
            row = reach(16 * d + i)
            sxc[d, 0, i] = row[0:32].astype(BF)
            for part in range(3):
                sxm[d, part, i] = row[32 + 32 * part : 64 + 32 * part].astype(BF)
            sxc[d, 1, i] = row[128:160].astype(BF)

        @pl.when(near[d])
        def _():
            for e in range(2):
                send_corner(d, e).start()
            for part in range(3):
                send_middle(d, part).start()

        for e in range(2):

            @pl.when(far[d] & has[e])
            def _():
                send_corner_far(d, e).start()

            @pl.when(far[d] & jnp.logical_not(has[e]))
            def _():
                send_middle(d, 2 * e).start()

        @pl.when(far[d])
        def _():
            send_middle(d, 1).start()

    for i in range(4, 8):
        acc[i] = reach(i + 4)
    for e in range(2):
        sz[e, 1] = acc[4:8, 128 * e : 128 * e + 32].astype(BF)

        @pl.when(has[e])
        def _():
            send_rows(e, 1).start()

    for i in (0, 1, 2, 3, 8, 9, 10, 11):
        acc[i] = reach(i + 4)

    for d in range(2):
        for e in range(2):

            @pl.when(far[d] & has[e])
            def _():
                send_corner_far(d, 1 - e).wait_recv()
                sxm[d, 2 * e] = (
                    sxm[d, 2 * e].astype(F32) + ryc[d, 1 - e].astype(F32)
                ).astype(BF)
                send_middle(d, 2 * e).start()

    for d in range(2):
        first = 8 - 8 * d

        @pl.when(far[1 - d])
        def _():
            for e in range(2):
                sz[e, 2 - 2 * d] = acc[first : first + 4, 128 * e : 128 * e + 32].astype(BF)

        @pl.when(near[1 - d])
        def _():
            for e in range(2):
                send_corner(d, e).wait_recv()
                sz[e, 2 - 2 * d] = (
                    acc[first : first + 4, 128 * e : 128 * e + 32] + rxc[d, e].astype(F32)
                ).astype(BF)

        for e in range(2):

            @pl.when(has[e])
            def _():
                send_rows(e, 2 - 2 * d).start()

    for d in range(2):
        first = 8 - 8 * d
        for part in range(3):
            send_middle(d, part).wait_recv()
            at = 32 + 32 * part
            acc[first : first + 4, at : at + 32] += rxm[d, part].astype(F32)

    for d in range(2):
        for part in range(3):

            @pl.when(has[1 - d])
            def _():
                send_rows(d, part).wait_recv()

    def leave(i):
        return pltpu.make_async_copy(out_v.at[i], out_ref.at[i], out_sem.at[i])

    def finish(i, carry):
        factor = scale_v[i]
        part, at = i // 4, lax.rem(i, 4)
        for y in range(12):
            total = acc[i, 32 + 8 * y : 40 + 8 * y, :]
            if y >= 8:
                total += rz[0, part, at, 8 * (y - 8) : 8 * (y - 8) + 8, :].astype(F32)
            if y < 4:
                total += rz[1, part, at, 8 * y : 8 * y + 8, :].astype(F32)
            out_v[i, y] = (factor[:, y : y + 1] * total).astype(BF)
        leave(i).start()
        return carry

    lax.fori_loop(0, 12, finish, 0)

    for i in range(12):
        leave(i).wait()
    for d in range(2):
        for part in range(3):
            halo_x(d, part).wait_send()
            send_middle(d, part).wait_send()

        @pl.when(near[d])
        def _():
            for e in range(2):
                send_corner(d, e).wait_send()

        for e in range(2):

            @pl.when(has[e] & near[d])
            def _():
                halo_corner(e, d).wait_send()

            @pl.when(has[e] & far[d])
            def _():
                halo_corner_far(d, e).wait_send()
                send_corner_far(d, e).wait_send()

        @pl.when(has[d])
        def _():
            for a in range(3):
                halo_y(d, a).wait_send()
                send_rows(d, a).wait_send()


def fused(nx, ny, nodes, fit, xyz, idx, scale, cell, valid, radius):
    fields = nodes.shape[3]
    anywhere = pl.BlockSpec(memory_space=pl.ANY)
    dma = pltpu.SemaphoreType.DMA
    return pl.pallas_call(
        functools.partial(kernel, nx, ny),
        out_shape=jax.ShapeDtypeStruct((12, 12, 8, fields), BF),
        in_specs=[anywhere] * 8,
        out_specs=anywhere,
        scratch_shapes=[
            pltpu.VMEM((5, 5, NSUB, fields), BF),
            pltpu.VMEM((K, PATCHES, KP), BF),
            pltpu.VMEM((3, PATCHES, K), F32),
            pltpu.VMEM((PATCHES, K), jnp.int32),
            pltpu.VMEM((12, 8, 12), F32),
            pltpu.VMEM((3, PATCHES, KL), F32),
            pltpu.VMEM((PATCHES, KS, 128), jnp.int32),
            pltpu.VMEM((3, KS * PATCHES, 128), F32),
            pltpu.VMEM((9 * SLAB, KL), BF),
            pltpu.VMEM((PATCHES, 9 * SLAB, KL), BF),
            pltpu.VMEM((PATCHES, KS, 9 * NSUB), BF),
            pltpu.VMEM((160, KL), BF),
            pltpu.VMEM((PATCHES, 10, SLAB, fields), BF),
            pltpu.VMEM((12, 160, fields), F32),
            pltpu.VMEM((2, 2, 4, 32, fields), BF),
            pltpu.VMEM((2, 3, 4, 32, fields), BF),
            pltpu.VMEM((2, 3, 4, 32, fields), BF),
            pltpu.VMEM((2, 2, 4, 32, fields), BF),
            pltpu.VMEM((2, 2, 4, 32, fields), BF),
            pltpu.VMEM((2, 3, 4, 32, fields), BF),
            pltpu.VMEM((2, 3, 4, 32, fields), BF),
            pltpu.VMEM((12, 12, 8, fields), BF),
            pltpu.SMEM((1, 3, 1, PATCHES), jnp.int32),
            pltpu.SMEM((1, 1, PATCHES), jnp.int32),
            pltpu.SMEM((1, 1, PATCHES), F32),
            dma((10,)),
            dma((2, 3)),
            dma((2, 3)),
            dma((2, 3)),
            dma((2, 3)),
            dma((2, 2)),
            dma((2, 2)),
            dma((2, 2)),
            dma((2, 2)),
            dma((2, 2)),
            dma((2, 2)),
            dma((2, 2)),
            dma((2, 2)),
            dma((2, 3)),
            dma((2, 3)),
            dma((2, 3)),
            dma((2, 3)),
            dma((12,)),
        ],
        compiler_params=pltpu.CompilerParams(
            collective_id=0, has_side_effects=True, vmem_limit_bytes=56 * 1024 * 1024
        ),
        name="fit_and_blend",
    )(nodes, fit, xyz, idx, scale, cell, valid, radius)


def local(
    nx,
    ny,
    node_values,
    fit_ops,
    node_xyz,
    patch_nodes,
    patch_valid,
    patch_cell,
    patch_radius,
    cell_scale,
):
    return fused(
        nx,
        ny,
        node_values,
        jnp.transpose(fit_ops[0, 0], (2, 0, 1)),
        jnp.transpose(node_xyz[0, 0], (1, 0, 2)),
        patch_nodes[0, 0],
        jnp.transpose(cell_scale, (0, 2, 1)),
        jnp.transpose(patch_cell, (0, 3, 1, 2)),
        patch_valid,
        patch_radius,
    )


def solution(mesh):
    placed = (
        P("gx", "gy", None, None),
        P("gx", "gy", None, None, None),
        P("gx", "gy", None, None, None),
        P("gx", "gy", None, None),
        P("gx", "gy", None),
        P("gx", "gy", None, None),
        P("gx", "gy", None),
        P("gx", "gy", None),
    )
    return jax.shard_map(
        functools.partial(local, mesh.shape["gx"], mesh.shape["gy"]),
        mesh=mesh,
        in_specs=placed,
        out_specs=P("gx", "gy", None, None),
        check_vma=False,
    )
```

```python
import functools

import jax
import jax.numpy as jnp
from jax import lax
from jax.experimental import pallas as pl
from jax.experimental.pallas import tpu as pltpu
from jax.sharding import PartitionSpec as P

EXPONENTS = (
    (0, 0, 0),
    (1, 0, 0),
    (0, 1, 0),
    (0, 0, 1),
    (2, 0, 0),
    (1, 1, 0),
    (1, 0, 1),
    (0, 2, 0),
    (0, 1, 1),
    (0, 0, 2),
    (3, 0, 0),
    (2, 1, 0),
    (2, 0, 1),
    (1, 2, 0),
    (1, 1, 1),
    (1, 0, 2),
    (0, 3, 0),
    (0, 2, 1),
    (0, 1, 2),
    (0, 0, 3),
)

K = 300
KS = 304
KP = 320
KL = 384
NSUB = 128
PATCHES = 8
RUN = 8
SLAB = 48
BF = jnp.bfloat16
F32 = jnp.float32


def remote(src, dst, send, recv, axis, target):
    return pltpu.make_async_remote_copy(
        src_ref=src,
        dst_ref=dst,
        send_sem=send,
        recv_sem=recv,
        device_id={axis: target},
        device_id_type=pl.DeviceIdType.MESH,
    )


def kernel(
    nx,
    ny,
    nodes_hbm,
    fit_hbm,
    xyz_hbm,
    idx_hbm,
    scale_hbm,
    cell_hbm,
    valid_hbm,
    radius_hbm,
    out_ref,
    nbr,
    fit_v,
    xyz_v,
    idx_v,
    scale_v,
    xyz_p,
    idx_b,
    ops_f,
    design,
    weights,
    onehot,
    place,
    samples,
    slabs,
    acc,
    sxc,
    sxm,
    sz,
    rxc,
    ryc,
    rxm,
    rz,
    out_v,
    cell_ref,
    valid_ref,
    radius_ref,
    local_sem,
    hz_send,
    hz_recv,
    hx_send,
    hx_recv,
    hf_send,
    hf_recv,
    hg_send,
    hg_recv,
    cc_send,
    cc_recv,
    cy_send,
    cy_recv,
    cm_send,
    cm_recv,
    cz_send,
    cz_recv,
    out_sem,
):
    gx, gy = lax.axis_index("gx"), lax.axis_index("gy")
    left, right = lax.rem(gx + nx - 1, nx), lax.rem(gx + 1, nx)
    sides_x = (left, right)
    far = (lax.rem(gx, RUN) == 0, lax.rem(gx, RUN) == RUN - 1)
    near = tuple(jnp.logical_not(f) for f in far)
    has = (gy > 0, gy < ny - 1)
    sides_y = (jnp.maximum(gy - 1, 0), jnp.minimum(gy + 1, ny - 1))

    barrier = pltpu.get_barrier_semaphore()
    for side in sides_x:
        pl.semaphore_signal(
            barrier, inc=1, device_id={"gx": side}, device_id_type=pl.DeviceIdType.MESH
        )
    for d in range(2):

        @pl.when(has[d])
        def _():
            pl.semaphore_signal(
                barrier,
                inc=1,
                device_id={"gy": sides_y[d]},
                device_id_type=pl.DeviceIdType.MESH,
            )

    own = [
        pltpu.make_async_copy(
            nodes_hbm.at[a], nbr.at[a + 1, pl.ds(1, 3)], local_sem.at[7 + a]
        )
        for a in range(3)
    ]
    fetches = [
        pltpu.make_async_copy(idx_hbm, idx_v, local_sem.at[0]),
        pltpu.make_async_copy(xyz_hbm, xyz_v, local_sem.at[1]),
        pltpu.make_async_copy(fit_hbm, fit_v, local_sem.at[2]),
        pltpu.make_async_copy(scale_hbm, scale_v, local_sem.at[3]),
        pltpu.make_async_copy(cell_hbm, cell_ref, local_sem.at[4]),
        pltpu.make_async_copy(valid_hbm, valid_ref, local_sem.at[5]),
        pltpu.make_async_copy(radius_hbm, radius_ref, local_sem.at[6]),
    ]
    for fetch in own + fetches:
        fetch.start()
    for fetch in own:
        fetch.wait()
    waits = 2 + jnp.where(gy > 0, 1, 0) + jnp.where(gy < ny - 1, 1, 0)
    pl.semaphore_wait(barrier, waits)

    def halo_y(d, a):
        return remote(
            nbr.at[a + 1, 1 + 2 * d],
            nbr.at[a + 1, 4 - 4 * d],
            hz_send.at[d, a],
            hz_recv.at[d, a],
            "gy",
            sides_y[d],
        )

    def halo_x(d, b):
        return remote(
            nbr.at[1 + 2 * d, b + 1],
            nbr.at[4 - 4 * d, b + 1],
            hx_send.at[d, b],
            hx_recv.at[d, b],
            "gx",
            sides_x[d],
        )

    def halo_corner(e, d):
        return remote(
            nbr.at[1 + 2 * d, 4 * e],
            nbr.at[4 - 4 * d, 4 * e],
            hf_send.at[e, d],
            hf_recv.at[e, d],
            "gx",
            sides_x[d],
        )

    def halo_corner_far(d, e):
        return remote(
            nbr.at[4 * d, 1 + 2 * e],
            nbr.at[4 * d, 4 - 4 * e],
            hg_send.at[d, e],
            hg_recv.at[d, e],
            "gy",
            sides_y[e],
        )

    for a in (0, 2, 1):
        for d in range(2):

            @pl.when(has[d])
            def _():
                halo_y(d, a).start()

        for d in range(2):
            halo_x(d, a).start()

    for e in range(2):

        @pl.when(jnp.logical_not(has[e]))
        def _():
            for a in range(5):
                nbr[a, 4 * e] = jnp.zeros(nbr.shape[2:], BF)
            rz[1 - e] = jnp.zeros(rz.shape[1:], BF)

    for i in (0, 1, 4, 5, 6):
        fetches[i].wait()
    xyz_p[...] = jnp.zeros(xyz_p.shape, F32)
    xyz_p[:, :, 0:K] = xyz_v[...]
    entry = jnp.concatenate(
        [idx_v[...], jnp.zeros((PATCHES, KL - K), jnp.int32)], 1
    )
    sub = entry >> 7
    a = (sub * 52) >> 8
    patch = lax.broadcasted_iota(jnp.int32, (PATCHES, KL), 0)
    home = jnp.zeros((PATCHES, KL), jnp.int32)
    count = jnp.zeros((PATCHES, KL), jnp.int32)
    for p in range(PATCHES):
        corner = (cell_ref[0, 0, 0, p] // 4) * 3 + cell_ref[0, 1, 0, p] // 4
        home = jnp.where(patch == p, corner, home)
        count = jnp.where(patch == p, valid_ref[0, 0, p], count)
    entry = ((sub - 2 * a - home) << 7) + (entry & 127)
    slot = lax.broadcasted_iota(jnp.int32, (PATCHES, KL), 1)
    entry = jnp.where(slot < count, entry, -1)
    columns = jnp.transpose(entry.astype(F32))
    for p in range(PATCHES):
        idx_b[p] = jnp.broadcast_to(columns[0:KS, p : p + 1], (KS, 128)).astype(jnp.int32)

    for p in range(PATCHES):
        slabs[p, 9] = jnp.zeros((SLAB, slabs.shape[3]), BF)
        samples[p, KS:KL] = jnp.zeros((KL - KS, samples.shape[2]), BF)

    lane = lax.broadcasted_iota(jnp.int32, (1, KL), 1)
    owner, within = lane // SLAB, lane % SLAB
    target = jnp.zeros((1, KL), jnp.int32)
    for p in range(PATCHES):
        start = cell_ref[0, 1, 0, p] * 8 + cell_ref[0, 2, 0, p]
        target = jnp.where(owner == p, start, target)
    target = target + (within // 4) * 8 + within % 4
    target = jnp.where(within < 36, target, -1)
    rows = lax.broadcasted_iota(jnp.int32, (160, KL), 0)
    place[...] = jnp.where(rows == target, 1.0, 0.0).astype(BF)

    fetches[2].wait()
    for t in range(3):
        ops_f[t, K * 8 : KS * 8, :] = jnp.zeros(((KS - K) * 8, 128), F32)
    ops_f[2, :, 64:128] = jnp.zeros((KS * 8, 64), F32)

    def widen(i, carry):
        block = fit_v[pl.ds(i * 20, 20)].astype(F32).reshape(160, KP)
        at = pl.multiple_of(i * 160, 8)
        ops_f[0, pl.ds(at, 160), :] = block[:, 0:128]
        ops_f[1, pl.ds(at, 160), :] = block[:, 128:256]
        ops_f[2, pl.ds(at, 160), 0:64] = block[:, 256:320]
        return carry

    lax.fori_loop(0, K // 20, widen, 0)

    def prepare(p, carry):
        inverse = 1.0 / jnp.full((1, 128), radius_ref[0, 0, p], F32)
        inverse3 = jnp.concatenate([inverse] * 3, 1)
        x = xyz_p[0, pl.ds(p, 1), :] * inverse3
        y = xyz_p[1, pl.ds(p, 1), :] * inverse3
        z = xyz_p[2, pl.ds(p, 1), :] * inverse3
        row = lax.broadcasted_iota(jnp.int32, (SLAB, 128), 0)
        ey = (row // 4 - 4).astype(F32) * inverse
        ez = ((row % 4).astype(F32) - 1.5) * inverse
        ey3 = jnp.concatenate([ey] * 3, 1)
        ez3 = jnp.concatenate([ez] * 3, 1)
        away_yz = (ey3 - y) * (ey3 - y) + (ez3 - z) * (ez3 - z)
        flat = ey * ey + ez * ez
        tail = lax.broadcasted_iota(jnp.int32, (1, 128), 1) - (K - 256)

        def powers(base, which):
            result = jnp.zeros(jnp.broadcast_shapes(base.shape, (1, 128)), F32)
            raised = [jnp.ones_like(base), base, base * base, base * base * base]
            for power in range(4):
                hit = jnp.zeros((1, 128), jnp.bool_)
                for slot, exponent in enumerate(EXPONENTS):
                    if exponent[which] == power:
                        hit = hit | (tail == slot)
                result = jnp.where(hit, raised[power], result)
            return result

        mono_yz = powers(ey, 1) * powers(ez, 2)
        ops = jnp.concatenate(
            [ops_f[t, pl.ds(p, KS, stride=8), :].astype(BF) for t in range(3)], 1
        )
        ops = jnp.concatenate([ops, jnp.zeros((KL - KS, KL), BF)], 0)
        for group in range(3):
            for i in range(3 * group, 3 * group + 3):
                ex = (i - 4) * inverse
                ex3 = jnp.concatenate([ex] * 3, 1)
                s = (ex3 - x) * (ex3 - x) + away_yz
                cubic = s * s * lax.rsqrt(jnp.maximum(s, 1e-30))
                mono = powers(ex, 0) * mono_yz
                last = jnp.where(tail < 0, cubic[:, 256:384], mono)
                design[SLAB * i : SLAB * i + SLAB, 0:256] = cubic[:, 0:256].astype(BF)
                design[SLAB * i : SLAB * i + SLAB, 256:384] = last.astype(BF)
            w = lax.dot_general(
                design[3 * SLAB * group : 3 * SLAB * group + 3 * SLAB, :],
                ops,
                (((1,), (1,)), ((), ())),
                preferred_element_type=F32,
            )
            for j in range(3):
                i = 3 * group + j
                ex = (i - 4) * inverse
                rho = jnp.sqrt(ex * ex + flat)
                rest = jnp.maximum(1.0 - rho, 0.0)
                rest = rest * rest
                blend = rest * rest * (4.0 * rho + 1.0)
                blend = jnp.where(row < 36, blend, 0.0)
                weights[p, SLAB * i : SLAB * i + SLAB, :] = (
                    w[SLAB * j : SLAB * j + SLAB] * jnp.concatenate([blend] * 3, 1)
                ).astype(BF)

        entry = idx_b[p]
        node = (entry & 127).astype(F32).astype(BF)
        block = (entry >> 7).astype(F32).astype(BF)
        lanes = lax.broadcasted_iota(jnp.int32, (KS, 128), 1).astype(F32).astype(BF)
        match = jnp.where(node == lanes, block, jnp.full((KS, 128), -1.0, BF))
        one, zero = jnp.full((KS, 128), 1.0, BF), jnp.zeros((KS, 128), BF)
        for t in range(9):
            onehot[p, :, 128 * t : 128 * t + 128] = jnp.where(
                match == jnp.full((KS, 128), t, BF), one, zero
            )
        return carry

    lax.fori_loop(0, 4, prepare, 0)
    for e in range(2):
        for d in range(2):

            @pl.when(has[e] & near[d])
            def _():
                halo_y(1 - e, 2 * d).wait_recv()
                halo_corner(e, d).start()

            @pl.when(has[e] & far[d])
            def _():
                halo_x(1 - d, 2 * e).wait_recv()
                halo_corner_far(d, e).start()

    lax.fori_loop(4, PATCHES, prepare, 0)

    fetches[3].wait()
    for d in range(2):
        halo_x(d, 1).wait_recv()
        for e in range(2):
            @pl.when(near[1 - d] | jnp.logical_not(has[e]))
            def _():
                halo_x(d, 2 * e).wait_recv()

            @pl.when(has[e] & far[d])
            def _():
                halo_y(1 - e, 2 * d).wait_recv()

            @pl.when(has[e] & near[d])
            def _():
                halo_corner(e, 1 - d).wait_recv()

            @pl.when(has[e] & far[d])
            def _():
                halo_corner_far(d, 1 - e).wait_recv()

    for e in range(2):

        @pl.when(has[e])
        def _():
            halo_y(1 - e, 1).wait_recv()

    for p in range(PATCHES):
        home_x, home_y = cell_ref[0, 0, 0, p] // 4, cell_ref[0, 1, 0, p] // 4
        window = jnp.concatenate(
            [
                nbr[home_x + a, pl.ds(home_y, 3)].reshape(3 * NSUB, nbr.shape[3])
                for a in range(3)
            ],
            0,
        )
        samples[p, 0:KS] = jnp.dot(
            onehot[p], window, preferred_element_type=F32
        ).astype(BF)

    def evaluate(i, carry):
        for j in range(4):
            p = 4 * i + j
            terms = jnp.dot(weights[p], samples[p], preferred_element_type=F32)
            slabs[p, 0:9] = terms.astype(BF).reshape(9, SLAB, terms.shape[1])
        return carry

    lax.fori_loop(0, 2, evaluate, 0)

    def reach(x):
        parts = []
        for p in range(PATCHES):
            at = x - cell_ref[0, 0, 0, p]
            at = jnp.where((at >= 0) & (at < 9), at, 9)
            parts.append(slabs[p, at])
        return jnp.dot(
            place[...], jnp.concatenate(parts, 0), preferred_element_type=F32
        )

    def send_corner(d, e):
        return remote(
            sxc.at[d, e], rxc.at[d, e], cc_send.at[d, e], cc_recv.at[d, e], "gx", sides_x[d]
        )

    def send_corner_far(d, e):
        return remote(
            sxc.at[d, e], ryc.at[d, e], cy_send.at[d, e], cy_recv.at[d, e], "gy", sides_y[e]
        )

    def send_middle(d, part):
        return remote(
            sxm.at[d, part],
            rxm.at[d, part],
            cm_send.at[d, part],
            cm_recv.at[d, part],
            "gx",
            sides_x[d],
        )

    def send_rows(d, part):
        return remote(
            sz.at[d, part],
            rz.at[d, part],
            cz_send.at[d, part],
            cz_recv.at[d, part],
            "gy",
            sides_y[d],
        )

    for d in range(2):
        for i in range(4):
            row = reach(16 * d + i)
            sxc[d, 0, i] = row[0:32].astype(BF)
            for part in range(3):
                sxm[d, part, i] = row[32 + 32 * part : 64 + 32 * part].astype(BF)
            sxc[d, 1, i] = row[128:160].astype(BF)

        @pl.when(near[d])
        def _():
            for e in range(2):
                send_corner(d, e).start()
            for part in range(3):
                send_middle(d, part).start()

        for e in range(2):

            @pl.when(far[d] & has[e])
            def _():
                send_corner_far(d, e).start()

            @pl.when(far[d] & jnp.logical_not(has[e]))
            def _():
                send_middle(d, 2 * e).start()

        @pl.when(far[d])
        def _():
            send_middle(d, 1).start()

    for i in range(4, 8):
        acc[i] = reach(i + 4)
    for e in range(2):
        sz[e, 1] = acc[4:8, 128 * e : 128 * e + 32].astype(BF)

        @pl.when(has[e])
        def _():
            send_rows(e, 1).start()

    for i in (0, 1, 2, 3, 8, 9, 10, 11):
        acc[i] = reach(i + 4)

    for d in range(2):
        for e in range(2):

            @pl.when(far[d] & has[e])
            def _():
                send_corner_far(d, 1 - e).wait_recv()
                sxm[d, 2 * e] = (
                    sxm[d, 2 * e].astype(F32) + ryc[d, 1 - e].astype(F32)
                ).astype(BF)
                send_middle(d, 2 * e).start()

    for d in range(2):
        first = 8 - 8 * d

        @pl.when(far[1 - d])
        def _():
            for e in range(2):
                sz[e, 2 - 2 * d] = acc[first : first + 4, 128 * e : 128 * e + 32].astype(BF)

        @pl.when(near[1 - d])
        def _():
            for e in range(2):
                send_corner(d, e).wait_recv()
                sz[e, 2 - 2 * d] = (
                    acc[first : first + 4, 128 * e : 128 * e + 32] + rxc[d, e].astype(F32)
                ).astype(BF)

        for e in range(2):

            @pl.when(has[e])
            def _():
                send_rows(e, 2 - 2 * d).start()

    def leave(i):
        return pltpu.make_async_copy(out_v.at[i], out_ref.at[i], out_sem.at[i])

    def finish(part, d):
        def one(at, carry):
            i = 4 * part + at
            factor = scale_v[i]
            for y in range(12):
                total = acc[i, 32 + 8 * y : 40 + 8 * y, :]
                third, row = y // 4, 8 * (y % 4)
                if d is not None:
                    total += rxm[d, third, at, row : row + 8, :].astype(F32)
                if third != 1:
                    total += rz[1 - third // 2, part, at, row : row + 8, :].astype(F32)
                out_v[i, y] = (factor[:, y : y + 1] * total).astype(BF)
            leave(i).start()
            return carry

        for e in range(2):

            @pl.when(has[1 - e])
            def _():
                send_rows(e, part).wait_recv()

        if d is not None:
            for third in range(3):
                send_middle(d, third).wait_recv()
        lax.fori_loop(0, 4, one, 0)

    finish(1, None)
    finish(0, 1)
    finish(2, 0)

    for i in range(12):
        leave(i).wait()
    for d in range(2):
        for part in range(3):
            halo_x(d, part).wait_send()
            send_middle(d, part).wait_send()

        @pl.when(near[d])
        def _():
            for e in range(2):
                send_corner(d, e).wait_send()

        for e in range(2):

            @pl.when(has[e] & near[d])
            def _():
                halo_corner(e, d).wait_send()

            @pl.when(has[e] & far[d])
            def _():
                halo_corner_far(d, e).wait_send()
                send_corner_far(d, e).wait_send()

        @pl.when(has[d])
        def _():
            for a in range(3):
                halo_y(d, a).wait_send()
                send_rows(d, a).wait_send()


def fused(nx, ny, nodes, fit, xyz, idx, scale, cell, valid, radius):
    fields = nodes.shape[3]
    anywhere = pl.BlockSpec(memory_space=pl.ANY)
    dma = pltpu.SemaphoreType.DMA
    return pl.pallas_call(
        functools.partial(kernel, nx, ny),
        out_shape=jax.ShapeDtypeStruct((12, 12, 8, fields), BF),
        in_specs=[anywhere] * 8,
        out_specs=anywhere,
        scratch_shapes=[
            pltpu.VMEM((5, 5, NSUB, fields), BF),
            pltpu.VMEM((K, PATCHES, KP), BF),
            pltpu.VMEM((3, PATCHES, K), F32),
            pltpu.VMEM((PATCHES, K), jnp.int32),
            pltpu.VMEM((12, 8, 12), F32),
            pltpu.VMEM((3, PATCHES, KL), F32),
            pltpu.VMEM((PATCHES, KS, 128), jnp.int32),
            pltpu.VMEM((3, KS * PATCHES, 128), F32),
            pltpu.VMEM((9 * SLAB, KL), BF),
            pltpu.VMEM((PATCHES, 9 * SLAB, KL), BF),
            pltpu.VMEM((PATCHES, KS, 9 * NSUB), BF),
            pltpu.VMEM((160, KL), BF),
            pltpu.VMEM((PATCHES, KL, fields), BF),
            pltpu.VMEM((PATCHES, 10, SLAB, fields), BF),
            pltpu.VMEM((12, 160, fields), F32),
            pltpu.VMEM((2, 2, 4, 32, fields), BF),
            pltpu.VMEM((2, 3, 4, 32, fields), BF),
            pltpu.VMEM((2, 3, 4, 32, fields), BF),
            pltpu.VMEM((2, 2, 4, 32, fields), BF),
            pltpu.VMEM((2, 2, 4, 32, fields), BF),
            pltpu.VMEM((2, 3, 4, 32, fields), BF),
            pltpu.VMEM((2, 3, 4, 32, fields), BF),
            pltpu.VMEM((12, 12, 8, fields), BF),
            pltpu.SMEM((1, 3, 1, PATCHES), jnp.int32),
            pltpu.SMEM((1, 1, PATCHES), jnp.int32),
            pltpu.SMEM((1, 1, PATCHES), F32),
            dma((10,)),
            dma((2, 3)),
            dma((2, 3)),
            dma((2, 3)),
            dma((2, 3)),
            dma((2, 2)),
            dma((2, 2)),
            dma((2, 2)),
            dma((2, 2)),
            dma((2, 2)),
            dma((2, 2)),
            dma((2, 2)),
            dma((2, 2)),
            dma((2, 3)),
            dma((2, 3)),
            dma((2, 3)),
            dma((2, 3)),
            dma((12,)),
        ],
        compiler_params=pltpu.CompilerParams(
            collective_id=0, has_side_effects=True, vmem_limit_bytes=56 * 1024 * 1024
        ),
        name="fit_and_blend",
    )(nodes, fit, xyz, idx, scale, cell, valid, radius)


def local(
    nx,
    ny,
    node_values,
    fit_ops,
    node_xyz,
    patch_nodes,
    patch_valid,
    patch_cell,
    patch_radius,
    cell_scale,
):
    return fused(
        nx,
        ny,
        node_values,
        jnp.transpose(fit_ops[0, 0], (2, 0, 1)),
        jnp.transpose(node_xyz[0, 0], (1, 0, 2)),
        patch_nodes[0, 0],
        jnp.transpose(cell_scale, (0, 2, 1)),
        jnp.transpose(patch_cell, (0, 3, 1, 2)),
        patch_valid,
        patch_radius,
    )


def solution(mesh):
    placed = (
        P("gx", "gy", None, None),
        P("gx", "gy", None, None, None),
        P("gx", "gy", None, None, None),
        P("gx", "gy", None, None),
        P("gx", "gy", None),
        P("gx", "gy", None, None),
        P("gx", "gy", None),
        P("gx", "gy", None),
    )
    return jax.shard_map(
        functools.partial(local, mesh.shape["gx"], mesh.shape["gy"]),
        mesh=mesh,
        in_specs=placed,
        out_specs=P("gx", "gy", None, None),
        check_vma=False,
    )
```

```python
import functools

import jax
import jax.numpy as jnp
from jax import lax
from jax.experimental import pallas as pl
from jax.experimental.pallas import tpu as pltpu
from jax.sharding import PartitionSpec as P

EXPONENTS = (
    (0, 0, 0),
    (1, 0, 0),
    (0, 1, 0),
    (0, 0, 1),
    (2, 0, 0),
    (1, 1, 0),
    (1, 0, 1),
    (0, 2, 0),
    (0, 1, 1),
    (0, 0, 2),
    (3, 0, 0),
    (2, 1, 0),
    (2, 0, 1),
    (1, 2, 0),
    (1, 1, 1),
    (1, 0, 2),
    (0, 3, 0),
    (0, 2, 1),
    (0, 1, 2),
    (0, 0, 3),
)

K = 300
KS = 304
KP = 320
KL = 384
NSUB = 128
PATCHES = 8
RUN = 8
SLAB = 48
BF = jnp.bfloat16
F32 = jnp.float32


def remote(src, dst, send, recv, axis, target):
    return pltpu.make_async_remote_copy(
        src_ref=src,
        dst_ref=dst,
        send_sem=send,
        recv_sem=recv,
        device_id={axis: target},
        device_id_type=pl.DeviceIdType.MESH,
    )


def kernel(
    nx,
    ny,
    nodes_hbm,
    fit_hbm,
    xyz_hbm,
    idx_hbm,
    scale_hbm,
    cell_hbm,
    valid_hbm,
    radius_hbm,
    out_ref,
    nbr,
    fit_v,
    xyz_v,
    idx_v,
    scale_v,
    xyz_p,
    idx_b,
    ops_f,
    design,
    weights,
    onehot,
    place,
    samples,
    slabs,
    acc,
    sxc,
    sxm,
    sz,
    rxc,
    ryc,
    rxm,
    rz,
    out_v,
    cell_ref,
    valid_ref,
    radius_ref,
    ready,
    local_sem,
    hz_send,
    hz_recv,
    hx_send,
    hx_recv,
    hf_send,
    hf_recv,
    hg_send,
    hg_recv,
    cc_send,
    cc_recv,
    cy_send,
    cy_recv,
    cm_send,
    cm_recv,
    cz_send,
    cz_recv,
    out_sem,
):
    gx, gy = lax.axis_index("gx"), lax.axis_index("gy")
    left, right = lax.rem(gx + nx - 1, nx), lax.rem(gx + 1, nx)
    sides_x = (left, right)
    far = (lax.rem(gx, RUN) == 0, lax.rem(gx, RUN) == RUN - 1)
    near = tuple(jnp.logical_not(f) for f in far)
    has = (gy > 0, gy < ny - 1)
    sides_y = (jnp.maximum(gy - 1, 0), jnp.minimum(gy + 1, ny - 1))

    barrier = pltpu.get_barrier_semaphore()
    pl.semaphore_signal(
        barrier, inc=1, device_id={"gx": left}, device_id_type=pl.DeviceIdType.MESH
    )

    @pl.when(near[1])
    def _():
        pl.semaphore_signal(
            barrier, inc=1, device_id={"gx": right}, device_id_type=pl.DeviceIdType.MESH
        )

    for d in range(2):

        @pl.when(has[d])
        def _():
            pl.semaphore_signal(
                barrier,
                inc=1,
                device_id={"gy": sides_y[d]},
                device_id_type=pl.DeviceIdType.MESH,
            )

    own = [
        pltpu.make_async_copy(
            nodes_hbm.at[a], nbr.at[a + 1, pl.ds(1, 3)], local_sem.at[7 + a]
        )
        for a in range(3)
    ]
    fetches = [
        pltpu.make_async_copy(idx_hbm, idx_v, local_sem.at[0]),
        pltpu.make_async_copy(xyz_hbm, xyz_v, local_sem.at[1]),
        pltpu.make_async_copy(fit_hbm, fit_v, local_sem.at[2]),
        pltpu.make_async_copy(scale_hbm, scale_v, local_sem.at[3]),
        pltpu.make_async_copy(cell_hbm, cell_ref, local_sem.at[4]),
        pltpu.make_async_copy(valid_hbm, valid_ref, local_sem.at[5]),
        pltpu.make_async_copy(radius_hbm, radius_ref, local_sem.at[6]),
    ]
    for fetch in own + fetches:
        fetch.start()
    waits = 1 + jnp.where(near[0], 1, 0)
    waits += jnp.where(gy > 0, 1, 0) + jnp.where(gy < ny - 1, 1, 0)
    pl.semaphore_wait(barrier, waits)

    @pl.when(far[1])
    def _():
        pl.semaphore_signal(
            ready, inc=1, device_id={"gx": right}, device_id_type=pl.DeviceIdType.MESH
        )

    for fetch in own:
        fetch.wait()


    def halo_y(d, a):
        return remote(
            nbr.at[a + 1, 1 + 2 * d],
            nbr.at[a + 1, 4 - 4 * d],
            hz_send.at[d, a],
            hz_recv.at[d, a],
            "gy",
            sides_y[d],
        )

    def halo_x(d, b):
        return remote(
            nbr.at[1 + 2 * d, b + 1],
            nbr.at[4 - 4 * d, b + 1],
            hx_send.at[d, b],
            hx_recv.at[d, b],
            "gx",
            sides_x[d],
        )

    def halo_corner(e, d):
        return remote(
            nbr.at[1 + 2 * d, 4 * e],
            nbr.at[4 - 4 * d, 4 * e],
            hf_send.at[e, d],
            hf_recv.at[e, d],
            "gx",
            sides_x[d],
        )

    def halo_corner_far(d, e):
        return remote(
            nbr.at[4 * d, 1 + 2 * e],
            nbr.at[4 * d, 4 - 4 * e],
            hg_send.at[d, e],
            hg_recv.at[d, e],
            "gy",
            sides_y[e],
        )

    for a in (0, 2, 1):
        for d in range(2):

            @pl.when(has[d])
            def _():
                halo_y(d, a).start()

        halo_x(1, a).start()

        @pl.when(near[0])
        def _():
            halo_x(0, a).start()


    for e in range(2):

        @pl.when(jnp.logical_not(has[e]))
        def _():
            for a in range(5):
                nbr[a, 4 * e] = jnp.zeros(nbr.shape[2:], BF)
            rz[1 - e] = jnp.zeros(rz.shape[1:], BF)

    for i in (0, 1, 4, 5, 6):
        fetches[i].wait()
    xyz_p[...] = jnp.zeros(xyz_p.shape, F32)
    xyz_p[:, :, 0:K] = xyz_v[...]
    entry = jnp.concatenate(
        [idx_v[...], jnp.zeros((PATCHES, KL - K), jnp.int32)], 1
    )
    sub = entry >> 7
    a = (sub * 52) >> 8
    patch = lax.broadcasted_iota(jnp.int32, (PATCHES, KL), 0)
    home = jnp.zeros((PATCHES, KL), jnp.int32)
    count = jnp.zeros((PATCHES, KL), jnp.int32)
    for p in range(PATCHES):
        corner = (cell_ref[0, 0, 0, p] // 4) * 3 + cell_ref[0, 1, 0, p] // 4
        home = jnp.where(patch == p, corner, home)
        count = jnp.where(patch == p, valid_ref[0, 0, p], count)
    entry = ((sub - 2 * a - home) << 7) + (entry & 127)
    slot = lax.broadcasted_iota(jnp.int32, (PATCHES, KL), 1)
    entry = jnp.where(slot < count, entry, -1)
    columns = jnp.transpose(entry.astype(F32))
    for p in range(PATCHES):
        idx_b[p] = jnp.broadcast_to(columns[0:KS, p : p + 1], (KS, 128)).astype(jnp.int32)

    for p in range(PATCHES):
        slabs[p, 9] = jnp.zeros((SLAB, slabs.shape[3]), BF)
        samples[p, KS:KL] = jnp.zeros((KL - KS, samples.shape[2]), BF)

    lane = lax.broadcasted_iota(jnp.int32, (1, KL), 1)
    owner, within = lane // SLAB, lane % SLAB
    target = jnp.zeros((1, KL), jnp.int32)
    for p in range(PATCHES):
        start = cell_ref[0, 1, 0, p] * 8 + cell_ref[0, 2, 0, p]
        target = jnp.where(owner == p, start, target)
    target = target + (within // 4) * 8 + within % 4
    target = jnp.where(within < 36, target, -1)
    rows = lax.broadcasted_iota(jnp.int32, (160, KL), 0)
    place[...] = jnp.where(rows == target, 1.0, 0.0).astype(BF)

    fetches[2].wait()
    for t in range(3):
        ops_f[t, K * 8 : KS * 8, :] = jnp.zeros(((KS - K) * 8, 128), F32)
    ops_f[2, :, 64:128] = jnp.zeros((KS * 8, 64), F32)

    def widen(i, carry):
        block = fit_v[pl.ds(i * 20, 20)].astype(F32).reshape(160, KP)
        at = pl.multiple_of(i * 160, 8)
        ops_f[0, pl.ds(at, 160), :] = block[:, 0:128]
        ops_f[1, pl.ds(at, 160), :] = block[:, 128:256]
        ops_f[2, pl.ds(at, 160), 0:64] = block[:, 256:320]
        return carry

    lax.fori_loop(0, K // 20, widen, 0)

    def prepare(p, carry):
        inverse = 1.0 / jnp.full((1, 128), radius_ref[0, 0, p], F32)
        inverse3 = jnp.concatenate([inverse] * 3, 1)
        x = xyz_p[0, pl.ds(p, 1), :] * inverse3
        y = xyz_p[1, pl.ds(p, 1), :] * inverse3
        z = xyz_p[2, pl.ds(p, 1), :] * inverse3
        row = lax.broadcasted_iota(jnp.int32, (SLAB, 128), 0)
        ey = (row // 4 - 4).astype(F32) * inverse
        ez = ((row % 4).astype(F32) - 1.5) * inverse
        ey3 = jnp.concatenate([ey] * 3, 1)
        ez3 = jnp.concatenate([ez] * 3, 1)
        away_yz = (ey3 - y) * (ey3 - y) + (ez3 - z) * (ez3 - z)
        flat = ey * ey + ez * ez
        tail = lax.broadcasted_iota(jnp.int32, (1, 128), 1) - (K - 256)

        def powers(base, which):
            result = jnp.zeros(jnp.broadcast_shapes(base.shape, (1, 128)), F32)
            raised = [jnp.ones_like(base), base, base * base, base * base * base]
            for power in range(4):
                hit = jnp.zeros((1, 128), jnp.bool_)
                for slot, exponent in enumerate(EXPONENTS):
                    if exponent[which] == power:
                        hit = hit | (tail == slot)
                result = jnp.where(hit, raised[power], result)
            return result

        mono_yz = powers(ey, 1) * powers(ez, 2)
        ops = jnp.concatenate(
            [ops_f[t, pl.ds(p, KS, stride=8), :].astype(BF) for t in range(3)], 1
        )
        ops = jnp.concatenate([ops, jnp.zeros((KL - KS, KL), BF)], 0)
        for group in range(3):
            for i in range(3 * group, 3 * group + 3):
                ex = (i - 4) * inverse
                ex3 = jnp.concatenate([ex] * 3, 1)
                s = (ex3 - x) * (ex3 - x) + away_yz
                cubic = s * s * lax.rsqrt(jnp.maximum(s, 1e-30))
                mono = powers(ex, 0) * mono_yz
                last = jnp.where(tail < 0, cubic[:, 256:384], mono)
                design[SLAB * i : SLAB * i + SLAB, 0:256] = cubic[:, 0:256].astype(BF)
                design[SLAB * i : SLAB * i + SLAB, 256:384] = last.astype(BF)
            w = lax.dot_general(
                design[3 * SLAB * group : 3 * SLAB * group + 3 * SLAB, :],
                ops,
                (((1,), (1,)), ((), ())),
                preferred_element_type=F32,
            )
            for j in range(3):
                i = 3 * group + j
                ex = (i - 4) * inverse
                rho = jnp.sqrt(ex * ex + flat)
                rest = jnp.maximum(1.0 - rho, 0.0)
                rest = rest * rest
                blend = rest * rest * (4.0 * rho + 1.0)
                blend = jnp.where(row < 36, blend, 0.0)
                weights[p, SLAB * i : SLAB * i + SLAB, :] = (
                    w[SLAB * j : SLAB * j + SLAB] * jnp.concatenate([blend] * 3, 1)
                ).astype(BF)

        entry = idx_b[p]
        node = (entry & 127).astype(F32).astype(BF)
        block = (entry >> 7).astype(F32).astype(BF)
        lanes = lax.broadcasted_iota(jnp.int32, (KS, 128), 1).astype(F32).astype(BF)
        match = jnp.where(node == lanes, block, jnp.full((KS, 128), -1.0, BF))
        one, zero = jnp.full((KS, 128), 1.0, BF), jnp.zeros((KS, 128), BF)
        for t in range(9):
            onehot[p, :, 128 * t : 128 * t + 128] = jnp.where(
                match == jnp.full((KS, 128), t, BF), one, zero
            )
        return carry

    lax.fori_loop(0, 5, prepare, 0)

    @pl.when(far[0])
    def _():
        pl.semaphore_wait(ready, 1)
        for a in (0, 2, 1):
            halo_x(0, a).start()

    lax.fori_loop(5, 6, prepare, 0)
    for e in range(2):
        for d in range(2):

            @pl.when(has[e] & near[d])
            def _():
                halo_y(1 - e, 2 * d).wait_recv()
                halo_corner(e, d).start()

    lax.fori_loop(6, PATCHES, prepare, 0)
    for e in range(2):
        for d in range(2):

            @pl.when(has[e] & far[d])
            def _():
                halo_x(1 - d, 2 * e).wait_recv()
                halo_corner_far(d, e).start()

    fetches[3].wait()
    for d in range(2):
        halo_x(d, 1).wait_recv()
        for e in range(2):
            @pl.when(near[1 - d] | jnp.logical_not(has[e]))
            def _():
                halo_x(d, 2 * e).wait_recv()

            @pl.when(has[e] & far[d])
            def _():
                halo_y(1 - e, 2 * d).wait_recv()

            @pl.when(has[e] & near[d])
            def _():
                halo_corner(e, 1 - d).wait_recv()

            @pl.when(has[e] & far[d])
            def _():
                halo_corner_far(d, 1 - e).wait_recv()

    for e in range(2):

        @pl.when(has[e])
        def _():
            halo_y(1 - e, 1).wait_recv()

    for p in range(PATCHES):
        home_x, home_y = cell_ref[0, 0, 0, p] // 4, cell_ref[0, 1, 0, p] // 4
        window = jnp.concatenate(
            [
                nbr[home_x + a, pl.ds(home_y, 3)].reshape(3 * NSUB, nbr.shape[3])
                for a in range(3)
            ],
            0,
        )
        samples[p, 0:KS] = jnp.dot(
            onehot[p], window, preferred_element_type=F32
        ).astype(BF)

    def evaluate(i, carry):
        for j in range(4):
            p = 4 * i + j
            terms = jnp.dot(weights[p], samples[p], preferred_element_type=F32)
            slabs[p, 0:9] = terms.astype(BF).reshape(9, SLAB, terms.shape[1])
        return carry

    lax.fori_loop(0, 2, evaluate, 0)

    def reach(x):
        parts = []
        for p in range(PATCHES):
            at = x - cell_ref[0, 0, 0, p]
            at = jnp.where((at >= 0) & (at < 9), at, 9)
            parts.append(slabs[p, at])
        return jnp.dot(
            place[...], jnp.concatenate(parts, 0), preferred_element_type=F32
        )

    def send_corner(d, e):
        return remote(
            sxc.at[d, e], rxc.at[d, e], cc_send.at[d, e], cc_recv.at[d, e], "gx", sides_x[d]
        )

    def send_corner_far(d, e):
        return remote(
            sxc.at[d, e], ryc.at[d, e], cy_send.at[d, e], cy_recv.at[d, e], "gy", sides_y[e]
        )

    def send_middle(d, part):
        return remote(
            sxm.at[d, part],
            rxm.at[d, part],
            cm_send.at[d, part],
            cm_recv.at[d, part],
            "gx",
            sides_x[d],
        )

    def send_rows(d, part):
        return remote(
            sz.at[d, part],
            rz.at[d, part],
            cz_send.at[d, part],
            cz_recv.at[d, part],
            "gy",
            sides_y[d],
        )

    for d in range(2):
        for i in range(4):
            row = reach(16 * d + i)
            sxc[d, 0, i] = row[0:32].astype(BF)
            for part in range(3):
                sxm[d, part, i] = row[32 + 32 * part : 64 + 32 * part].astype(BF)
            sxc[d, 1, i] = row[128:160].astype(BF)

        @pl.when(near[d])
        def _():
            for e in range(2):
                send_corner(d, e).start()
            for part in range(3):
                send_middle(d, part).start()

        for e in range(2):

            @pl.when(far[d] & has[e])
            def _():
                send_corner_far(d, e).start()

            @pl.when(far[d] & jnp.logical_not(has[e]))
            def _():
                send_middle(d, 2 * e).start()

        @pl.when(far[d])
        def _():
            send_middle(d, 1).start()

    for i in range(4, 8):
        acc[i] = reach(i + 4)
    for e in range(2):
        sz[e, 1] = acc[4:8, 128 * e : 128 * e + 32].astype(BF)

        @pl.when(has[e])
        def _():
            send_rows(e, 1).start()

    for i in (0, 1, 2, 3, 8, 9, 10, 11):
        acc[i] = reach(i + 4)

    for d in range(2):
        first = 8 - 8 * d
        for e in range(2):

            @pl.when(has[e] & far[1 - d])
            def _():
                sz[e, 2 - 2 * d] = acc[first : first + 4, 128 * e : 128 * e + 32].astype(BF)
                send_rows(e, 2 - 2 * d).start()

    for d in range(2):
        for e in range(2):

            @pl.when(far[d] & has[e])
            def _():
                send_corner_far(d, 1 - e).wait_recv()
                sxm[d, 2 * e] = (
                    sxm[d, 2 * e].astype(F32) + ryc[d, 1 - e].astype(F32)
                ).astype(BF)
                send_middle(d, 2 * e).start()

    for d in range(2):
        first = 8 - 8 * d

        @pl.when(near[1 - d])
        def _():
            for e in range(2):
                send_corner(d, e).wait_recv()
                sz[e, 2 - 2 * d] = (
                    acc[first : first + 4, 128 * e : 128 * e + 32] + rxc[d, e].astype(F32)
                ).astype(BF)

        for e in range(2):

            @pl.when(has[e] & near[1 - d])
            def _():
                send_rows(e, 2 - 2 * d).start()

    def leave(i):
        return pltpu.make_async_copy(out_v.at[i], out_ref.at[i], out_sem.at[i])

    def finish(part, d):
        def one(at, carry):
            i = 4 * part + at
            factor = scale_v[i]
            for y in range(12):
                total = acc[i, 32 + 8 * y : 40 + 8 * y, :]
                third, row = y // 4, 8 * (y % 4)
                if d is not None:
                    total += rxm[d, third, at, row : row + 8, :].astype(F32)
                if third != 1:
                    total += rz[1 - third // 2, part, at, row : row + 8, :].astype(F32)
                out_v[i, y] = (factor[:, y : y + 1] * total).astype(BF)
            leave(i).start()
            return carry

        for e in range(2):

            @pl.when(has[1 - e])
            def _():
                send_rows(e, part).wait_recv()

        if d is not None:
            for third in range(3):
                send_middle(d, third).wait_recv()
        lax.fori_loop(0, 4, one, 0)

    finish(1, None)
    finish(0, 1)
    finish(2, 0)

    for i in range(12):
        leave(i).wait()
    for d in range(2):
        for part in range(3):
            halo_x(d, part).wait_send()
            send_middle(d, part).wait_send()

        @pl.when(near[d])
        def _():
            for e in range(2):
                send_corner(d, e).wait_send()

        for e in range(2):

            @pl.when(has[e] & near[d])
            def _():
                halo_corner(e, d).wait_send()

            @pl.when(has[e] & far[d])
            def _():
                halo_corner_far(d, e).wait_send()
                send_corner_far(d, e).wait_send()

        @pl.when(has[d])
        def _():
            for a in range(3):
                halo_y(d, a).wait_send()
                send_rows(d, a).wait_send()


def fused(nx, ny, nodes, fit, xyz, idx, scale, cell, valid, radius):
    fields = nodes.shape[3]
    anywhere = pl.BlockSpec(memory_space=pl.ANY)
    dma = pltpu.SemaphoreType.DMA
    return pl.pallas_call(
        functools.partial(kernel, nx, ny),
        out_shape=jax.ShapeDtypeStruct((12, 12, 8, fields), BF),
        in_specs=[anywhere] * 8,
        out_specs=anywhere,
        scratch_shapes=[
            pltpu.VMEM((5, 5, NSUB, fields), BF),
            pltpu.VMEM((K, PATCHES, KP), BF),
            pltpu.VMEM((3, PATCHES, K), F32),
            pltpu.VMEM((PATCHES, K), jnp.int32),
            pltpu.VMEM((12, 8, 12), F32),
            pltpu.VMEM((3, PATCHES, KL), F32),
            pltpu.VMEM((PATCHES, KS, 128), jnp.int32),
            pltpu.VMEM((3, KS * PATCHES, 128), F32),
            pltpu.VMEM((9 * SLAB, KL), BF),
            pltpu.VMEM((PATCHES, 9 * SLAB, KL), BF),
            pltpu.VMEM((PATCHES, KS, 9 * NSUB), BF),
            pltpu.VMEM((160, KL), BF),
            pltpu.VMEM((PATCHES, KL, fields), BF),
            pltpu.VMEM((PATCHES, 10, SLAB, fields), BF),
            pltpu.VMEM((12, 160, fields), F32),
            pltpu.VMEM((2, 2, 4, 32, fields), BF),
            pltpu.VMEM((2, 3, 4, 32, fields), BF),
            pltpu.VMEM((2, 3, 4, 32, fields), BF),
            pltpu.VMEM((2, 2, 4, 32, fields), BF),
            pltpu.VMEM((2, 2, 4, 32, fields), BF),
            pltpu.VMEM((2, 3, 4, 32, fields), BF),
            pltpu.VMEM((2, 3, 4, 32, fields), BF),
            pltpu.VMEM((12, 12, 8, fields), BF),
            pltpu.SMEM((1, 3, 1, PATCHES), jnp.int32),
            pltpu.SMEM((1, 1, PATCHES), jnp.int32),
            pltpu.SMEM((1, 1, PATCHES), F32),
            pltpu.SemaphoreType.REGULAR,
            dma((10,)),
            dma((2, 3)),
            dma((2, 3)),
            dma((2, 3)),
            dma((2, 3)),
            dma((2, 2)),
            dma((2, 2)),
            dma((2, 2)),
            dma((2, 2)),
            dma((2, 2)),
            dma((2, 2)),
            dma((2, 2)),
            dma((2, 2)),
            dma((2, 3)),
            dma((2, 3)),
            dma((2, 3)),
            dma((2, 3)),
            dma((12,)),
        ],
        compiler_params=pltpu.CompilerParams(
            collective_id=0, has_side_effects=True, vmem_limit_bytes=56 * 1024 * 1024
        ),
        name="fit_and_blend",
    )(nodes, fit, xyz, idx, scale, cell, valid, radius)


def local(
    nx,
    ny,
    node_values,
    fit_ops,
    node_xyz,
    patch_nodes,
    patch_valid,
    patch_cell,
    patch_radius,
    cell_scale,
):
    return fused(
        nx,
        ny,
        node_values,
        jnp.transpose(fit_ops[0, 0], (2, 0, 1)),
        jnp.transpose(node_xyz[0, 0], (1, 0, 2)),
        patch_nodes[0, 0],
        jnp.transpose(cell_scale, (0, 2, 1)),
        jnp.transpose(patch_cell, (0, 3, 1, 2)),
        patch_valid,
        patch_radius,
    )


def solution(mesh):
    placed = (
        P("gx", "gy", None, None),
        P("gx", "gy", None, None, None),
        P("gx", "gy", None, None, None),
        P("gx", "gy", None, None),
        P("gx", "gy", None),
        P("gx", "gy", None, None),
        P("gx", "gy", None),
        P("gx", "gy", None),
    )
    return jax.shard_map(
        functools.partial(local, mesh.shape["gx"], mesh.shape["gy"]),
        mesh=mesh,
        in_specs=placed,
        out_specs=P("gx", "gy", None, None),
        check_vma=False,
    )
```
